128 devices in a mesh: rep: 1, dp: 128 (over x, y, z, core).
Axes of the slice: x: 4, y: 4, z: 4, core: 2. Of those that a mesh axis runs over, the one named last changes fastest.
Arguments:
- x: bfloat16 [128, 1024, 1024], P(('rep', 'dp'))
- dy: bfloat16 [128, 1024, 1024], P(('rep', 'dp'))
- w_gate: bfloat16 [2, 1024, 3200], replicated
- w_up: bfloat16 [2, 1024, 3200], replicated
- w_down: bfloat16 [2, 3200, 1024], replicated
- m_w_gate: float32 [2, 1024, 3200], replicated
- m_w_up: float32 [2, 1024, 3200], replicated
- m_w_down: float32 [2, 3200, 1024], replicated
- v_w_gate: float32 [2, 1024, 3200], replicated
- v_w_up: float32 [2, 1024, 3200], replicated
- v_w_down: float32 [2, 3200, 1024], replicated
Outputs:
- output 1: bfloat16 [2, 1024, 3200], P('rep')
- output 2: bfloat16 [2, 1024, 3200], P('rep')
- output 3: bfloat16 [2, 3200, 1024], P('rep')
- output 4: float32 [2, 1024, 3200], P('rep')
- output 5: float32 [2, 1024, 3200], P('rep')
- output 6: float32 [2, 3200, 1024], P('rep')
- output 7: float32 [2, 1024, 3200], P('rep')
- output 8: float32 [2, 1024, 3200], P('rep')
- output 9: float32 [2, 3200, 1024], P('rep')
All inputs are finite; a program needn't handle non-finite values.
Results may differ from the reference program's by a relative error of at most 0.022.
Values are sent between devices in bfloat16 or wider.
A program may use at most 1.5 GiB of HBM per device.

```python
import jax
import jax.numpy as jnp
from jax import lax

SEQUENCES = 128
TOKENS = 1024
D = 1024
FF = 3200
LAYERS = 2
NAMES = ("w_gate", "w_up", "w_down")
SHAPES = {"w_gate": (LAYERS, D, FF), "w_up": (LAYERS, D, FF), "w_down": (LAYERS, FF, D)}


def bump(key, n, height):
    away = (jnp.arange(n, dtype=jnp.int32) - jax.random.randint(key, (), 0, n, jnp.int32)) % n
    return jnp.where(away < n // 8, height, 1.0)


def together(key, own, strength):
    shared = jax.random.normal(key, own.shape[1:], jnp.float32)
    return (own + strength * shared) * lax.rsqrt(1 + strength * strength)


def setup_inputs(seed: int = 0, part: int = 0) -> dict:
    kx, kdy, ka, kb, kz, kf, kh, kl, *keys = jax.random.split(jax.random.key(seed), 8 + 3 * len(NAMES))
    kx, kdy, ka, kb = (jax.random.fold_in(k, part) for k in (kx, kdy, ka, kb))
    kw, km, kv = (keys[i::3] for i in range(3))
    shape = (SEQUENCES, TOKENS, D)
    much_x, much_dy = jax.random.uniform(kz, (2,), jnp.float32, 0.0, 1.0)
    loud = 2.0 ** jax.random.uniform(jax.random.fold_in(kz, 1), (), jnp.float32, -1.0, 2.0)
    layers = 2.0 ** jax.random.uniform(kl, (LAYERS, 1, 1), jnp.float32, -1.0, 1.0)
    x = together(ka, jax.random.normal(kx, shape, jnp.float32), much_x) * bump(kf, D, 4.0)
    dy = together(kb, jax.random.normal(kdy, shape, jnp.float32), much_dy)
    drawn = {"x": x.astype(jnp.bfloat16), "dy": (loud * dy * (SEQUENCES * TOKENS) ** -0.5).astype(jnp.bfloat16)}
    for key, name in zip(kw, NAMES, strict=True):
        w = jax.random.normal(key, SHAPES[name], jnp.float32) * SHAPES[name][1] ** -0.5
        drawn[name] = (w * {"w_gate": 1.0, "w_up": bump(kh, FF, 4.0), "w_down": layers}[name]).astype(jnp.bfloat16)
    for key, name in zip(km, NAMES, strict=True):
        drawn[f"m_{name}"] = 0.1 * jax.random.normal(key, SHAPES[name], jnp.float32)
    for key, name in zip(kv, NAMES, strict=True):
        drawn[f"v_{name}"] = jax.random.uniform(key, SHAPES[name], jnp.float32, 0.005, 0.015)
    return drawn


def matmul(a, w):
    return jnp.dot(a, w, preferred_element_type=jnp.float32).astype(jnp.bfloat16)


def normed(h):
    wide = h.astype(jnp.float32)
    scale = lax.rsqrt(jnp.mean(wide**2, -1, keepdims=True) + 1e-6)
    return (wide * scale).astype(jnp.bfloat16)


def layer(h, w):
    a = normed(h)
    gate = jnp.dot(a, w["w_gate"], preferred_element_type=jnp.float32)
    up = jnp.dot(a, w["w_up"], preferred_element_type=jnp.float32)
    return h + matmul((jax.nn.silu(gate) * up).astype(jnp.bfloat16), w["w_down"])


def adamw(w, m, v, g):
    m = 0.9 * m + 0.1 * g
    v = 0.95 * v + 0.05 * g * g
    step = m * lax.rsqrt(v + 1e-8) + 0.1 * w
    return (w - 0.02 * step).astype(jnp.bfloat16), m, v


def clipped(gradients, sum_of_squares, count):
    factor = jnp.minimum(1.0, 0.5 * lax.rsqrt(sum_of_squares / count + 1e-30))
    return [g * factor for g in gradients]


def stack(weights, h):
    return lax.scan(lambda h, w: (layer(h, w), None), h, weights)[0]


def reference(x, dy, w_gate, w_up, w_down, m_w_gate, m_w_up, m_w_down, v_w_gate, v_w_up, v_w_down):
    weights = dict(zip(NAMES, (w_gate, w_up, w_down), strict=True))

    def take(so_far, sequence):
        h, by_y = sequence
        _, back = jax.vjp(lambda w: stack(w, h), weights)
        return jax.tree.map(lambda total, term: total + term.astype(jnp.float32), so_far, back(by_y)[0]), None

    none_yet = {name: jnp.zeros(w.shape, jnp.float32) for name, w in weights.items()}
    by_weights, _ = lax.scan(take, none_yet, (x, dy))
    gradients = [by_weights[name].astype(jnp.bfloat16).astype(jnp.float32) for name in NAMES]
    gradients = clipped(gradients, sum(jnp.sum(g * g) for g in gradients), sum(g.size for g in gradients))
    new = [
        adamw(w.astype(jnp.float32), m, v, g)
        for w, m, v, g in zip((w_gate, w_up, w_down), (m_w_gate, m_w_up, m_w_down), (v_w_gate, v_w_up, v_w_down), gradients, strict=True)
    ]
    return tuple(one[which] for which in range(3) for one in new)
```

```python
import functools

import jax
import jax.numpy as jnp
from jax import lax
from jax.experimental import pallas as pl
from jax.experimental.pallas import tpu as pltpu
from jax.sharding import PartitionSpec as P

LANES, BLOCK, TILE, SIDE, WIDE, SIX = 128, 256, 512, 1024, 3200, 6
START, WAIT = True, False
MESH = pl.DeviceIdType.MESH
ANY = pl.BlockSpec(memory_space=pl.ANY)
ROWS, HALF, QUARTER = 25600, 12800, 6400
STEPS = SIX
SLOTS, ASLOTS = 2, 3
SCOPES = WAIT


def coords():
    me = lax.axis_index("dp")
    return me, lax.rem(me, 2), (lax.div(me, 32), lax.rem(lax.div(me, 8), 4), lax.rem(lax.div(me, 2), 4))


def across(d):
    me, _, xyz = coords()
    c, stride = xyz[d // 2], (32, 8, 2)[d // 2]
    if d % 2:
        return me + (3 - 2 * c) * stride, lax.div(c, 2)
    return me + (1 - 2 * lax.rem(c, 2)) * stride, lax.rem(lax.div(c + 1, 2), 2)


def al(v, n=8):
    return pl.multiple_of(v, n)


def colors(body):
    @pl.loop(0, 5)
    def _(j):
        body(j, 4)

    body(5, 5)


def at(device):
    return {"dp": device}


class Comm:
    def __init__(self, refs, g, slots):
        self.__dict__.update(refs)
        self.g, self.slots, self.aslots = g, slots, ASLOTS

    def tables(self):
        pairs = [across(d) for d in range(SIX)]
        self.others, self.sides = [o for o, _ in pairs], [side for _, side in pairs]

    def pick(self, values, m, j, k):
        d = j + (m + k - 1) % SIX
        if isinstance(d, int):
            return values[d % SIX]
        d = lax.rem(d, SIX)
        value = values[0]
        for i in range(1, SIX):
            value = jnp.where(d == i, values[i], value)
        return value

    def other(self, m, j, k):
        return self.pick(self.others, m, j, k)

    def side(self, m, j, k):
        return self.pick(self.sides, m, j, k)

    def sent(self, j, n, k):
        return j * 1536 + (0 if k % 2 else n // 2)

    def rdma(self, m, j, n, k, device):
        s, h = m % self.slots, n >> k
        rows = pl.ds(al(j * 2048 + (n - (n >> (k - 1)))), h)
        mine = pl.ds(al(self.sent(j, n, k)), h)
        return pltpu.make_async_remote_copy(self.O.at[s, mine], self.R.at[s, rows], self.ss.at[s, j, k - 1], self.rs.at[s, j, k - 1], at(device), MESH)

    def pair(self, m, j, n, h, device):
        rows = pl.ds(al(h * QUARTER + j * SIDE), n // 2)
        return pltpu.make_async_remote_copy(self.OUT.at[rows], self.RP.at[rows], self.ps.at[j, h], self.pr.at[j, h], at(device), MESH)

    def add(self, m, k):
        s = m % self.slots

        def body(j, slabs):
            n = TILE * slabs
            got = self.rdma(m, j, n, k, self.other(m, j, k))
            got.wait()
            base, fb = j * 2048 + (n - (n >> (k - 1))), j * SIDE
            if k < STEPS:
                h = n >> (k + 1)
                device, side = self.other(m, j, k + 1), self.side(m, j, k + 1)
                step = min(h, 32 * slabs)

                @pl.loop(0, h // step)
                def _(i):
                    o = (1 - side) * h + i * step
                    total = self.F[s, pl.ds(al(fb + o), step)] + self.R[s, pl.ds(al(base + o), step)].astype(jnp.float32)
                    self.O[s, pl.ds(al(self.sent(j, n, k + 1) + i * step), step)] = total.astype(jnp.bfloat16)

                self.rdma(m, j, n, k + 1, device).start()

                @pl.loop(0, h // step)
                def _(i):
                    o = side * h + i * step
                    total = self.F[s, pl.ds(al(fb + o), step)] + self.R[s, pl.ds(al(base + o), step)].astype(jnp.float32)
                    self.F[s, pl.ds(al(fb + i * step), step)] = total

            else:
                h = n >> k
                total = self.F[s, pl.ds(al(fb), h)] + self.R[s, pl.ds(al(base), h)].astype(jnp.float32)
                total = total.astype(jnp.bfloat16)
                self.A[m % self.aslots, pl.ds(al(self.row(m, j, n, k)), h)] = total
                self.gather(m, j, n, k).start()
                wide = total.astype(jnp.float32)
                self.SQ[0] += jnp.sum((wide * wide).reshape(h // 8, 8, LANES), 0)

        if k == STEPS and m >= self.aslots:
            for d in range(SIX):
                pl.semaphore_wait(self.acredit.at[d], 1)
        colors(body)
        if k == STEPS and m + self.slots < SIX:
            self.tell(self.credit)

    def tell(self, credit):
        for d in range(SIX):
            pl.semaphore_signal(credit.at[d], inc=1, device_id=at(across(d)[0]), device_id_type=MESH)

    def row(self, m, j, n, k, flip=WAIT):
        row = j * SIDE
        for i in range(1, k + 1):
            side = self.side(m, j, i)
            if flip and i == k:
                side = 1 - side
            row = row + side * (QUARTER if i == 1 else n >> i)
        return row

    def gather(self, m, j, n, k):
        part = self.A.at[m % self.aslots, pl.ds(al(self.row(m, j, n, k)), n >> k)]
        return pltpu.make_async_remote_copy(part, part, self.gs.at[m, j, k - 1], self.gr.at[m, j, k - 1], at(self.other(m, j, k)), MESH)

    def store(self, m, j, n, q, away):
        me, core, _ = coords()
        k, flip = ((2, WAIT), (2, START), (1, START))[q]
        row = self.row(m, j, n, k, flip)
        part = self.A.at[m % self.aslots, pl.ds(al(row), n >> k)]
        to = self.g.at[pl.ds(al(m * ROWS + core * HALF + row), n >> k)]
        if not away:
            return pltpu.make_async_copy(part, to, self.gl.at[m, j, q])
        return pltpu.make_async_remote_copy(part, to, self.ds.at[m, j, q], self.dr.at[m, j, q], at(me + 1 - 2 * core), MESH)

    def back(self, m, k):
        def body(j, slabs):
            n = TILE * slabs
            self.gather(m, j, n, k + 1).wait()
            if k:
                self.gather(m, j, n, k).start()
            if k <= 2:
                for away in (WAIT, START):
                    self.store(m, j, n, 2 - k, away).start()

        colors(body)

    def free(self, m):
        def body(j, slabs):
            for q in range(3):
                self.store(m, j, TILE * slabs, q, WAIT).wait()
                self.store(m, j, TILE * slabs, q, START).wait_send()

        colors(body)
        if m + self.aslots < SIX:
            self.tell(self.acredit)

    def finish(self, m):
        def body(j, slabs):
            for q in range(3):
                self.store(m, j, TILE * slabs, q, START).wait_recv()

        colors(body)

    def squares(self, i):
        me, core, _ = coords()

        def copy(i):
            device = across(i - 1)[0] if i else me + 1 - 2 * core
            return pltpu.make_async_remote_copy(self.SQ.at[i], self.SQR.at[i], self.qs.at[i], self.qr.at[i], at(device), MESH)

        if i:
            copy(i - 1).wait()
            self.SQ[i] = self.SQ[i - 1] + self.SQR[i - 1]
        if i < 7:
            copy(i).start()


def tiles(body):
    @pl.loop(0, SIX)
    def _(i):
        body(i, TILE)

    body(jnp.int32(SIX), LANES)


def span(i, width):
    return pl.ds(pl.multiple_of(i * TILE, LANES), width)


def dot_t(a, b):
    return lax.dot_general(a, b, (((1,), (1,)), ((), ())), preferred_element_type=jnp.float32)


def go(copies, start):
    for c in copies:
        c.start() if start else c.wait()


def scale_of(wide):
    return lax.rsqrt(jnp.mean(wide * wide, -1, keepdims=START) + 1e-6)


def forward_kernel(x, dy, wg, wu, wd, a0_t, act0, gate, up, h1, a1_t, dy_t, act1, by_gate, by_up, XV, DY, AV, HV, TV, WS, WD, DT, ACT, ST, SB, sem, ws, ds, st, sb):
    def weights(layer, i, width, start):
        s = lax.rem(i, 2)
        go([pltpu.make_async_copy(w.at[layer, :, span(i, width)], WS.at[s, k, :, pl.ds(0, width)], ws.at[s, k]) for k, w in enumerate((wg, wu))], start)

    def downs(i, width, start):
        s = lax.rem(i, 2)
        go([pltpu.make_async_copy(wd.at[1, span(i, width), :], DT.at[s, pl.ds(0, width)], ds.at[s])], start)

    def saved(i, width, start):
        s = lax.rem(i, 2)
        go([pltpu.make_async_copy(ST.at[s, k, :, pl.ds(0, width)], o.at[:, span(i, width)], st.at[s, k]) for k, o in enumerate((gate, up))], start)

    def results(i, width, start):
        s = lax.rem(i, 2)
        go([pltpu.make_async_copy(SB.at[s, k, :, pl.ds(0, width)], o.at[:, span(i, width)], sb.at[s, k]) for k, o in enumerate((act1, by_gate, by_up))], start)

    def norm(states):
        for r in range(4):
            rows = slice(BLOCK * r, BLOCK * r + BLOCK)
            wide = states[rows].astype(jnp.float32)
            AV[rows] = (wide * scale_of(wide)).astype(jnp.bfloat16)

    def turn(a, t, i):
        TV[t, :, pl.ds(pl.multiple_of(i * LANES, LANES), LANES)] = a[pl.ds(pl.multiple_of(i * LANES, LANES), LANES), :].T

    x_in, dy_in, wd_in = (pltpu.make_async_copy(a, b, sem.at[k]) for k, (a, b) in enumerate(((x, XV), (dy, DY), (wd.at[0], WD))))
    x_in.start()
    weights(0, jnp.int32(0), TILE, START)
    weights(0, jnp.int32(1), TILE, START)
    wd_in.start()
    dy_in.start()
    x_in.wait()
    norm(XV)

    def first(i, width):
        s = lax.rem(i, 2)
        weights(0, i, width, WAIT)

        @pl.when(i >= 2)
        def _():
            saved(i - 2, TILE, WAIT)

        g = jnp.dot(AV[...], WS[s, 0, :, 0:width], preferred_element_type=jnp.float32)
        u = jnp.dot(AV[...], WS[s, 1, :, 0:width], preferred_element_type=jnp.float32)
        ST[s, 0, :, 0:width] = g
        ST[s, 1, :, 0:width] = u
        saved(i, width, START)
        ACT[:, span(i, width)] = (g * jax.nn.sigmoid(g) * u).astype(jnp.bfloat16)
        turn(AV, 0, i)
        if width == TILE:

            @pl.when(i < 4)
            def _():
                weights(0, i + 2, TILE, START)

            @pl.when(i == 4)
            def _():
                weights(0, jnp.int32(SIX), LANES, START)

    tiles(first)
    turn(AV, 0, 7)
    for i in range(2):
        weights(1, jnp.int32(i), TILE, START)
        downs(jnp.int32(i), TILE, START)
    outs = [pltpu.make_async_copy(TV.at[0], a0_t, sem.at[0]), pltpu.make_async_copy(ACT, act0, sem.at[3])]
    go(outs, START)
    wd_in.wait()
    dy_in.wait()

    @pl.loop(0, 2)
    def _(i):
        cols = pl.ds(pl.multiple_of(i * TILE, TILE), TILE)
        y = jnp.dot(ACT[...], WD[:, cols], preferred_element_type=jnp.float32)
        HV[:, cols] = XV[:, cols] + y.astype(jnp.bfloat16)
        for k in range(4):
            turn(DY, 1, 4 * i + k)

    later = [pltpu.make_async_copy(HV, h1, sem.at[1]), pltpu.make_async_copy(TV.at[1], dy_t, sem.at[2])]
    go(later, START)
    norm(HV)
    go(outs, WAIT)

    def second(i, width):
        s = lax.rem(i, 2)
        weights(1, i, width, WAIT)
        downs(i, width, WAIT)

        @pl.when(i >= 2)
        def _():
            results(i - 2, TILE, WAIT)

        g = jnp.dot(AV[...], WS[s, 0, :, 0:width], preferred_element_type=jnp.float32)
        u = jnp.dot(AV[...], WS[s, 1, :, 0:width], preferred_element_type=jnp.float32)
        d = dot_t(DY[...], DT[s, 0:width]).astype(jnp.bfloat16).astype(jnp.float32)
        sig = jax.nn.sigmoid(g)
        silu = g * sig
        SB[s, 0, :, 0:width] = (silu * u).astype(jnp.bfloat16)
        SB[s, 1, :, 0:width] = (d * u * (sig * (1 + g * (1 - sig)))).astype(jnp.bfloat16)
        SB[s, 2, :, 0:width] = (d * silu).astype(jnp.bfloat16)
        results(i, width, START)
        turn(AV, 0, i)
        if width == TILE:

            @pl.when(i < 4)
            def _():
                weights(1, i + 2, TILE, START)
                downs(i + 2, TILE, START)

            @pl.when(i == 4)
            def _():
                weights(1, jnp.int32(SIX), LANES, START)
                downs(jnp.int32(SIX), LANES, START)

    tiles(second)
    turn(AV, 0, 7)
    outs = [pltpu.make_async_copy(TV.at[0], a1_t, sem.at[0])]
    go(outs, START)
    saved(jnp.int32(5), TILE, WAIT)
    saved(jnp.int32(SIX), LANES, WAIT)
    results(jnp.int32(5), TILE, WAIT)
    results(jnp.int32(SIX), LANES, WAIT)
    go(outs + later, WAIT)


def forward(x, dy, wg, wu, wd):
    b, f, dma = jnp.bfloat16, jnp.float32, pltpu.SemaphoreType.DMA
    square, wide = (SIDE, SIDE), (SIDE, WIDE)
    vm = pltpu.VMEM
    outs = [(square, b), (wide, b), (wide, f), (wide, f), (square, b), (square, b), (square, b), (wide, b), (wide, b), (wide, b)]
    scratch = [vm(square, b)] * 2 + [vm(square, b)] * 2 + [vm((2, *square), b), vm((2, 2, SIDE, TILE), b), vm((WIDE, SIDE), b), vm((2, TILE, SIDE), b)]
    scratch += [vm(wide, b), vm((2, 2, SIDE, TILE), f), vm((2, 3, SIDE, TILE), b), dma((4,)), dma((2, 2)), dma((2,)), dma((2, 2)), dma((2, 3))]
    a0_t, act0, gate, up, h1, a1_t, dy_t, act1, by_gate1, by_up1 = pl.pallas_call(
        forward_kernel,
        out_shape=[jax.ShapeDtypeStruct(s, t) for s, t in outs],
        in_specs=[ANY] * 5,
        out_specs=[ANY] * 10,
        scratch_shapes=scratch,
        compiler_params=pltpu.CompilerParams(vmem_limit_bytes=62 * 2**20),
        name="forward",
    )(x, dy, wg, wu, wd)
    return dy_t, a1_t, a0_t, act1, by_gate1, by_up1, act0, wg, wu, wd, gate, up, h1, dy


SCRATCH = (
    ("X", (SIDE, WIDE), jnp.bfloat16),
    ("L", (2, SIDE, SIDE), jnp.bfloat16),
    ("OUT", (HALF, LANES), jnp.bfloat16),
    ("RP", (HALF, LANES), jnp.bfloat16),
    ("O", (SLOTS, 9600, LANES), jnp.bfloat16),
    ("R", (SLOTS, HALF, LANES), jnp.bfloat16),
    ("F", (SLOTS, QUARTER, LANES), jnp.float32),
    ("A", (ASLOTS, HALF, LANES), jnp.bfloat16),
    ("SQ", (8, 8, LANES), jnp.float32),
    ("SQR", (7, 8, LANES), jnp.float32),
    ("DA", (SIDE, SIDE), jnp.float32),
    ("WT", (2, SIDE, 640), jnp.bfloat16),
    ("BY", (SIDE, SIDE), jnp.bfloat16),
    ("GU", (2, 2, SIDE, BLOCK), jnp.float32),
    ("WD", (2, BLOCK, SIDE), jnp.bfloat16),
    ("DS", (2, SIDE, BLOCK), jnp.bfloat16),
)
SEMAPHORES = (
    ("ss", (SLOTS, SIX, SIX)), ("rs", (SLOTS, SIX, SIX)), ("ps", (SIX, 2)), ("pr", (SIX, 2)), ("gs", (SIX, SIX, SIX)), ("gr", (SIX, SIX, SIX)),
    ("gl", (SIX, SIX, 3)), ("ds", (SIX, SIX, 3)), ("dr", (SIX, SIX, 3)), ("qs", (7,)), ("qr", (7,)), ("xs", (SIX,)), ("ls", (2,)),
    ("wts", (2,)), ("hs", (2,)), ("gus", (2, 3)), ("dus", (2,)),
)


def gradients_kernel(*refs, order):
    dy_t, a1_t, a0_t, act1, by_gate1, by_up1, act0, w_gate, w_up, w_down, gate, up, h1, dy = refs[:14]
    g, factor, by_up0 = refs[14:17]
    r = dict(zip([s[0] for s in SCRATCH + SEMAPHORES] + ["credit", "acredit", "pcredit"], refs[17:], strict=START))
    X, L, OUT, RP, O, F, DA, WT, BY, GU, WD, DS = (r[n] for n in ("X", "L", "OUT", "RP", "O", "F", "DA", "WT", "BY", "GU", "WD", "DS"))
    comm = Comm(r, g, SLOTS)
    me, core, _ = coords()
    partner = me + 1 - 2 * core
    left_of = (0, 1, 1, 0, 1, 1)
    rights = (act1, by_gate1, by_up1, act0, None, by_up0)

    def left(a, i):
        return pltpu.make_async_copy(a, L.at[i], r["ls"].at[i])

    def right(m, j, slabs):
        cols = pl.ds(al(j * TILE, LANES), LANES * slabs)
        return pltpu.make_async_copy(rights[m].at[:, cols], X.at[:, cols], r["xs"].at[j])

    def row_tile(which, j):
        cols = pl.ds(al(j * TILE, LANES), 640)
        slot = lax.rem(j, 2)
        return pltpu.make_async_copy((w_up, w_gate)[which].at[1, :, cols], WT.at[slot], r["wts"].at[slot])

    def hidden(t, width, start):
        s, cols = lax.rem(t, 2), pl.ds(al(t * BLOCK, LANES), width)
        copies = [pltpu.make_async_copy(a.at[:, cols], GU.at[s, k, :, pl.ds(0, width)], r["gus"].at[s, k]) for k, a in enumerate((gate, up))]
        go(copies + [pltpu.make_async_copy(w_down.at[0, cols, :], WD.at[s, pl.ds(0, width)], r["gus"].at[s, 2])], start)

    def put(t, width, start):
        s, cols = lax.rem(t, 2), pl.ds(al(t * BLOCK, LANES), width)
        go([pltpu.make_async_copy(DS.at[s, :, pl.ds(0, width)], by_up0.at[:, cols], r["dus"].at[s])], start)

    left(dy_t, 0).start()
    colors(lambda j, slabs: right(0, j, slabs).start())
    left(a1_t, 1).start()
    dy_in = pltpu.make_async_copy(dy, BY, r["hs"].at[0])
    h_in = pltpu.make_async_copy(h1, L.at[0], r["hs"].at[1])
    dy_in.start()
    row_tile(0, 0).start()
    hidden(0, BLOCK, START)
    hidden(1, BLOCK, START)
    comm.tables()
    barrier = pltpu.get_barrier_semaphore()
    for d in range(SIX):
        pl.semaphore_signal(barrier, inc=1, device_id=at(across(d)[0]), device_id_type=MESH)
    pl.semaphore_signal(barrier, inc=1, device_id=at(partner), device_id_type=MESH)
    r["SQ"][0] = jnp.zeros((8, LANES), jnp.float32)
    for b in range(4):
        DA[BLOCK * b : BLOCK * b + BLOCK] = jnp.zeros((BLOCK, SIDE), jnp.float32)
    pl.semaphore_wait(barrier, 7)

    def dot(m, row, rows, j, slabs):
        return jnp.dot(
            L[left_of[m], pl.ds(al(row, BLOCK), rows), :],
            X[:, pl.ds(al(j * TILE, TILE), LANES * slabs)],
            preferred_element_type=jnp.float32,
        )

    def theirs(m):
        if m == 0:
            left(dy_t, 0).wait()
        if m == 1:
            left(a1_t, 1).wait()
        if m == 4:
            left(a0_t, 1).wait()
        if m:
            pl.semaphore_wait(r["pcredit"], 1)

        def body(j, slabs):
            n = TILE * slabs
            if m != 4:
                right(m, j, slabs).wait()
            if m:
                for h in range(2):
                    comm.pair(m, j, n, h, partner).wait_send()
            res = dot(m, (1 - core) * TILE, TILE, j, slabs).astype(jnp.bfloat16)
            for h in range(2):
                for s in range(slabs):
                    OUT[pl.ds(al(h * QUARTER + j * SIDE + s * BLOCK), BLOCK)] = res[h * BLOCK : h * BLOCK + BLOCK, s * LANES : s * LANES + LANES]
                comm.pair(m, j, n, h, partner).start()

        colors(body)

    def ours(m, out):
        slot = m % SLOTS
        if out and m >= SLOTS:
            for d in range(SIX):
                pl.semaphore_wait(r["credit"].at[d], 1)

        def body(j, slabs):
            n = TILE * slabs
            device, side = comm.other(m, j, 1), comm.side(m, j, 1)
            h = 1 - side if out else side
            comm.pair(m, j, n, h, partner).wait_recv()
            res = dot(m, core * TILE + h * BLOCK, BLOCK, j, slabs)
            for s in range(slabs):
                total = res[:, s * LANES : s * LANES + LANES] + RP[pl.ds(al(h * QUARTER + j * SIDE + s * BLOCK), BLOCK)].astype(jnp.float32)
                if out:
                    O[slot, pl.ds(al(comm.sent(j, n, 1) + s * BLOCK), BLOCK)] = total.astype(jnp.bfloat16)
                else:
                    F[slot, pl.ds(al(j * SIDE + s * BLOCK), BLOCK)] = total
            if out:
                comm.rdma(m, j, n, 1, device).start()
            elif m in (0, 1, 4):
                right(m + 1, j, slabs).start()

        colors(body)
        if not out:
            if m < 5:
                pl.semaphore_signal(r["pcredit"], inc=1, device_id=at(partner), device_id_type=MESH)
            if m == 0:
                h_in.start()
            if m == 2:
                left(a0_t, 1).start()

    def by_normed(i):
        which, part = divmod(i, 3)

        def body(j, slabs):
            cols = pl.ds(al(j * TILE, LANES), LANES * slabs)
            if which:
                right(1, j, slabs).wait()
            row_tile(which, j).wait()
            if isinstance(j, int):
                if which == 0:
                    row_tile(1, 0).start()
            else:
                row_tile(which, j + 1).start()

            @pl.loop(0, 2)
            def _(half):
                rows = pl.ds(al(half * TILE, TILE), TILE)
                DA[rows] += dot_t(X[rows, cols], WT[lax.rem(j, 2), :, 0 : LANES * slabs])

            right(3 if which else 1, j, slabs).start()

        if part == 2:
            body(5, 5)
        else:

            @pl.loop(3 * part, 3 + 2 * part)
            def _(j):
                body(j, 4)

    def normed_back():
        dy_in.wait()
        h_in.wait()
        for b in range(4):
            rows = slice(BLOCK * b, BLOCK * b + BLOCK)
            wide = L[0, rows].astype(jnp.float32)
            scale = scale_of(wide)
            d = DA[rows].astype(jnp.bfloat16).astype(jnp.float32)
            through = d * scale - wide * (scale * scale * scale * jnp.mean(d * wide, -1, keepdims=START))
            BY[rows] = BY[rows] + through.astype(jnp.bfloat16)
        for b in range(4):
            rows = slice(BLOCK * b, BLOCK * b + BLOCK)
            L[0, :, rows] = BY[rows].T

    def by_hidden(i):
        def body(t, width):
            s = lax.rem(t, 2)
            hidden(t, width, WAIT)
            d = dot_t(BY[...], WD[s, 0:width]).astype(jnp.bfloat16).astype(jnp.float32)
            gt = GU[s, 0, :, 0:width]
            sig = jax.nn.sigmoid(gt)
            X[:, pl.ds(al(t * BLOCK, LANES), width)] = (d * GU[s, 1, :, 0:width] * (sig * (1 + gt * (1 - sig)))).astype(jnp.bfloat16)

            @pl.when(t >= 2)
            def _():
                put(t - 2, BLOCK, WAIT)

            DS[s, :, 0:width] = (d * (gt * sig)).astype(jnp.bfloat16)
            put(t, width, START)
            if width == BLOCK:

                @pl.when(t < 10)
                def _():
                    hidden(t + 2, BLOCK, START)

                @pl.when(t == 10)
                def _():
                    hidden(12, LANES, START)

        if i < 3:

            @pl.loop(4 * i, 4 * i + 4)
            def _(t):
                body(t, BLOCK)

        else:
            body(jnp.int32(12), LANES)
            put(11, BLOCK, WAIT)
            put(12, LANES, WAIT)

    def run(kind, m, k):
        if kind == "theirs":
            theirs(m)
        elif kind == "out":
            ours(m, START)
        elif kind == "stay":
            ours(m, WAIT)
        elif kind == "normed":
            by_normed(m)
        elif kind == "back_normed":
            normed_back()
        elif kind == "hidden":
            by_hidden(m)
        elif kind == "add":
            comm.add(m, k)
        elif kind == "back":
            comm.back(m, k)
        elif kind == "free":
            comm.free(m)
        elif kind == "sq":
            comm.squares(m)

    for item in order:
        if SCOPES:
            with jax.named_scope("_".join(str(i) for i in item)):
                run(*item)
        else:
            run(*item)
    for m in range(SIX):
        comm.finish(m)

    def last(j, slabs):
        for h in range(2):
            comm.pair(5, j, TILE * slabs, h, partner).wait_send()

    colors(last)
    total = jnp.sum(jnp.sum(r["SQ"][7], 1, keepdims=START), 0, keepdims=START)
    count = SIX * ROWS * LANES
    factor[...] = jnp.broadcast_to(jnp.minimum(1.0, 0.5 * lax.rsqrt(total / count + 1e-30)), (8, LANES))


def summed_gradients(order, *args):
    dma = pltpu.SemaphoreType.DMA
    regular = pltpu.SemaphoreType.REGULAR
    return pl.pallas_call(
        functools.partial(gradients_kernel, order=order),
        out_shape=(jax.ShapeDtypeStruct((SIX * ROWS, LANES), jnp.bfloat16), jax.ShapeDtypeStruct((8, LANES), jnp.float32), jax.ShapeDtypeStruct((SIDE, WIDE), jnp.bfloat16)),
        in_specs=[ANY] * 14,
        out_specs=[ANY, pl.BlockSpec(memory_space=pltpu.VMEM), ANY],
        scratch_shapes=[pltpu.VMEM(shape, t) for _, shape, t in SCRATCH] + [dma(shape) for _, shape in SEMAPHORES] + [regular((SIX,)), regular((SIX,)), regular],
        compiler_params=pltpu.CompilerParams(collective_id=0, has_side_effects=START, vmem_limit_bytes=67043328),
        name="gradients",
    )(*args)


CHOICES = (
    144476525018746880, 437236407134593730, 7892504941168264, 949859321295931548,
    970449292296088485, 34617268361661,
)


def steps():
    compute = []
    for m in range(SIX):
        compute += [(kind, m, -1) for kind in ("theirs", "out", "stay")]
        if m == 2:
            compute += [("normed", i, -1) for i in range(SIX)] + [("back_normed", 0, -1)]
        if m == 3:
            compute += [("hidden", i, -1) for i in range(4)]
    chains = [compute]
    for m in range(SIX):
        chains.append([("add", m, k) for k in range(1, 7)] + [("back", m, k) for k in range(5, -1, -1)] + [("free", m, 0)])
    chains.append([("sq", i, 0) for i in range(8)])
    chains = [iter(chain) for chain in chains]
    count = 115
    return [next(chains[CHOICES[i // 20] >> (3 * (i % 20)) & 7]) for i in range(count)]


ROWS_A = 64
DEEP = 4


def adam_kernel(factor, g, *refs):
    ins, outs = (refs[0:3], refs[3:SIX], refs[SIX:9]), (refs[9:12], refs[12:15], refs[15:18])
    gf, gt, *rest = refs[18:]
    flat_in, turned_in, flat_out, turned_out, got, put = rest[0:3], rest[3:SIX], rest[SIX:9], rest[9:12], rest[12], rest[13]
    per = SIDE // ROWS_A
    flat, tiles = 4 * per, 4 * per + 50

    def pieces(i, act):
        for n in range(3):
            first, count = (0, per) if n == 0 else (2 * per, per) if n == 1 else (4 * per, 25)

            @pl.when((i >= first) & (i < first + 2 * count))
            def _():
                layer, t = lax.div(i - first, count), lax.rem(i - first, count)
                chunk = ((1 - layer) * 3 + (1, 2, 0)[n]) * 4
                rows = LANES if n == 2 else ROWS_A
                place = (layer, pl.ds(pl.multiple_of(t * rows, rows), rows))
                if n == 2:
                    act(n, place, g.at[pl.ds(chunk, 4), t])
                else:
                    part = BLOCK // ROWS_A
                    act(n, place, g.at[chunk + lax.div(t, part), :, pl.ds(pl.multiple_of(lax.rem(t, part) * ROWS_A, ROWS_A), ROWS_A)])

    def load(i, start):
        slot = lax.rem(i, DEEP)

        def act(n, place, grads):
            copies = [pltpu.make_async_copy(grads, (gt if n == 2 else gf).at[slot], got.at[slot, 3])]
            for k in range(3):
                buffer = (turned_in if n == 2 else flat_in)[k]
                copies.append(pltpu.make_async_copy(ins[k][n].at[place], buffer.at[slot], got.at[slot, k]))
            for c in copies:
                c.start() if start else c.wait()

        pieces(i, act)

    def store(i, start):
        slot = lax.rem(i, DEEP)

        def act(n, place, grads):
            for k in range(3):
                buffer = (turned_out if n == 2 else flat_out)[k]
                c = pltpu.make_async_copy(buffer.at[slot], outs[k][n].at[place], put.at[slot, k])
                c.start() if start else c.wait()

        pieces(i, act)

    def compute(i, turned):
        slot = lax.rem(i, DEEP)
        w, m, v = turned_in if turned else flat_in
        w_out, m_out, v_out = turned_out if turned else flat_out
        f = factor[0:1, 0:1] if turned else factor[0:1, :]
        for s in range(4 if turned else 25):
            if turned:
                piece = gt[slot, s].astype(jnp.float32).T
                where = (slot, slice(None), slice(BLOCK * s, BLOCK * s + BLOCK))
            else:
                piece = gf[slot, s].astype(jnp.float32)
                where = (slot, slice(None), slice(LANES * s, LANES * s + LANES))
            piece = piece * f
            new_m = 0.9 * m[where] + 0.1 * piece
            new_v = 0.95 * v[where] + 0.05 * piece * piece
            wide = w[where].astype(jnp.float32)
            step = new_m * lax.rsqrt(new_v + 1e-8) + 0.1 * wide
            m_out[where] = new_m
            v_out[where] = new_v
            w_out[where] = (wide - 0.02 * step).astype(jnp.bfloat16)

    for i in range(DEEP - 1):
        load(jnp.int32(i), START)

    @pl.loop(0, tiles)
    def _(i):
        @pl.when(i + DEEP - 1 < tiles)
        def _():
            load(i + DEEP - 1, START)

        load(i, WAIT)

        @pl.when(i >= DEEP)
        def _():
            store(i - DEEP, WAIT)

        @pl.when(i < flat)
        def _():
            compute(i, WAIT)

        @pl.when(i >= flat)
        def _():
            compute(i, START)

        store(i, START)

    @pl.loop(tiles - DEEP, tiles)
    def _(i):
        store(i, WAIT)


def adam(factor, g, weights, m, v):
    arrays = (*weights, *m, *v)
    flat, turned = (DEEP, ROWS_A, WIDE), (DEEP, LANES, SIDE)
    types = (jnp.bfloat16, jnp.float32, jnp.float32)
    return pl.pallas_call(
        adam_kernel,
        out_shape=tuple(jax.ShapeDtypeStruct(a.shape, a.dtype) for a in arrays),
        in_specs=[pl.BlockSpec(memory_space=pltpu.VMEM), ANY] + [ANY] * 9,
        out_specs=(ANY,) * 9,
        scratch_shapes=[pltpu.VMEM((DEEP, 25, ROWS_A, LANES), jnp.bfloat16), pltpu.VMEM((DEEP, 4, BLOCK, LANES), jnp.bfloat16)]
        + [pltpu.VMEM(shape, t) for _ in range(2) for shape in (flat, turned) for t in types]
        + [pltpu.SemaphoreType.DMA((DEEP, 4)), pltpu.SemaphoreType.DMA((DEEP, 3))],
        compiler_params=pltpu.CompilerParams(vmem_limit_bytes=60 * 2**20),
        name="adam",
    )(factor, g.reshape(24, 25, BLOCK, LANES), *arrays)


def solution(mesh):
    order = steps()

    def step(x, dy, *arrays):
        weights, m, v = (arrays[i : i + 3] for i in (0, 3, SIX))
        g, factor, _ = summed_gradients(order, *forward(x[0], dy[0], *weights))
        return tuple(adam(factor, g, weights, m, v))

    return jax.shard_map(
        step,
        mesh=mesh,
        in_specs=(P(("rep", "dp"), None, None),) * 2 + (P(None, None, None),) * 9,
        out_specs=(P("rep", None, None),) * 9,
        check_vma=WAIT,
    )
```

```python
import functools

import jax
import jax.numpy as jnp
from jax import lax
from jax.experimental import pallas as pl
from jax.experimental.pallas import tpu as pltpu
from jax.sharding import PartitionSpec as P

LANES, BLOCK, TILE, SIDE, WIDE, SIX = 128, 256, 512, 1024, 3200, 6
START, WAIT = True, False
MESH = pl.DeviceIdType.MESH
ANY = pl.BlockSpec(memory_space=pl.ANY)
ROWS, HALF, QUARTER = 25600, 12800, 6400
STEPS = SIX
SLOTS, ASLOTS = 2, 3
SCOPES = WAIT


def coords():
    me = lax.axis_index("dp")
    return me, lax.rem(me, 2), (lax.div(me, 32), lax.rem(lax.div(me, 8), 4), lax.rem(lax.div(me, 2), 4))


def across(d):
    me, _, xyz = coords()
    c, stride = xyz[d // 2], (32, 8, 2)[d // 2]
    if d % 2:
        return me + (3 - 2 * c) * stride, lax.div(c, 2)
    return me + (1 - 2 * lax.rem(c, 2)) * stride, lax.rem(lax.div(c + 1, 2), 2)


def al(v, n=8):
    return pl.multiple_of(v, n)


def colors(body):
    @pl.loop(0, 5)
    def _(j):
        body(j, 4)

    body(5, 5)


def at(device):
    return {"dp": device}


class Comm:
    def __init__(self, refs, g):
        self.__dict__.update(refs)
        self.g = g

    def tables(self):
        pairs = [across(d) for d in range(SIX)]
        self.others, self.sides = [o for o, _ in pairs], [side for _, side in pairs]

    def pick(self, values, m, j, k):
        d = j + (m + k - 1) % SIX
        if isinstance(d, int):
            return values[d % SIX]
        d = lax.rem(d, SIX)
        value = values[0]
        for i in range(1, SIX):
            value = jnp.where(d == i, values[i], value)
        return value

    def other(self, m, j, k):
        return self.pick(self.others, m, j, k)

    def side(self, m, j, k):
        return self.pick(self.sides, m, j, k)

    def sent(self, j, n, k):
        return j * 1536 + (0 if k % 2 else n // 2)

    def rdma(self, m, j, n, k, device):
        s, h = m % SLOTS, n >> k
        rows = pl.ds(al(j * 2048 + (n - (n >> (k - 1)))), h)
        mine = pl.ds(al(self.sent(j, n, k)), h)
        return pltpu.make_async_remote_copy(self.O.at[s, mine], self.R.at[s, rows], self.ss.at[s, j], self.rs.at[s, j, k - 1], at(device), MESH)

    def pair(self, m, j, n, h, device):
        rows = pl.ds(al(h * QUARTER + j * SIDE), n // 2)
        return pltpu.make_async_remote_copy(self.OUT.at[rows], self.RP.at[rows], self.ps.at[j, h], self.pr.at[j, h], at(device), MESH)

    def add(self, m, k):
        s = m % SLOTS

        def body(j, slabs):
            n = TILE * slabs
            got = self.rdma(m, j, n, k, self.other(m, j, k))
            got.wait()
            base, fb = j * 2048 + (n - (n >> (k - 1))), j * SIDE
            if k < STEPS:
                h = n >> (k + 1)
                device, side = self.other(m, j, k + 1), self.side(m, j, k + 1)
                step = min(h, 32 * slabs)

                @pl.loop(0, h // step)
                def _(i):
                    o = (1 - side) * h + i * step
                    total = self.F[s, pl.ds(al(fb + o), step)] + self.R[s, pl.ds(al(base + o), step)].astype(jnp.float32)
                    self.O[s, pl.ds(al(self.sent(j, n, k + 1) + i * step), step)] = total.astype(jnp.bfloat16)

                self.rdma(m, j, n, k + 1, device).start()

                @pl.loop(0, h // step)
                def _(i):
                    o = side * h + i * step
                    total = self.F[s, pl.ds(al(fb + o), step)] + self.R[s, pl.ds(al(base + o), step)].astype(jnp.float32)
                    self.F[s, pl.ds(al(fb + i * step), step)] = total

            else:
                h = n >> k
                total = self.F[s, pl.ds(al(fb), h)] + self.R[s, pl.ds(al(base), h)].astype(jnp.float32)
                total = total.astype(jnp.bfloat16)
                self.A[m % ASLOTS, pl.ds(al(self.row(m, j, n, k)), h)] = total
                self.gather(m, j, n, k).start()
                wide = total.astype(jnp.float32)
                self.SQ[0] += jnp.sum((wide * wide).reshape(h // 8, 8, LANES), 0)

        if k == STEPS and m >= ASLOTS:
            for d in range(SIX):
                pl.semaphore_wait(self.acredit.at[d], 1)
        colors(body)
        if k == STEPS and m + SLOTS < SIX:
            self.tell(self.credit)

    def tell(self, credit):
        for d in range(SIX):
            pl.semaphore_signal(credit.at[d], inc=1, device_id=at(across(d)[0]), device_id_type=MESH)

    def row(self, m, j, n, k, flip=WAIT):
        row = j * SIDE
        for i in range(1, k + 1):
            side = self.side(m, j, i)
            if flip and i == k:
                side = 1 - side
            row = row + side * (QUARTER if i == 1 else n >> i)
        return row

    def gather(self, m, j, n, k):
        a = m % ASLOTS
        part = self.A.at[a, pl.ds(al(self.row(m, j, n, k)), n >> k)]
        return pltpu.make_async_remote_copy(part, part, self.gs.at[a, j], self.gr.at[a, j, k - 1], at(self.other(m, j, k)), MESH)

    def store(self, m, row, rows, away):
        me, core, _ = coords()
        a = m % ASLOTS
        part = self.A.at[a, pl.ds(al(row), rows)]
        to = self.g.at[pl.ds(al(m * ROWS + core * HALF + row), rows)]
        if not away:
            return pltpu.make_async_copy(part, to, self.gl.at[a])
        return pltpu.make_async_remote_copy(part, to, self.ds.at[a], self.dr.at[m], at(me + 1 - 2 * core), MESH)

    def back(self, m, k):
        def body(j, slabs):
            n = TILE * slabs
            self.gather(m, j, n, k + 1).wait()
            if k:
                self.gather(m, j, n, k).start()
            if k <= 2:
                half = 2 if k else 1
                row = self.row(m, j, n, half, k < 2)
                for away in (WAIT, START):
                    self.store(m, row, n >> half, away).start()

        colors(body)

    def free(self, m):
        self.store(m, 0, HALF, WAIT).wait()
        self.store(m, 0, HALF, START).wait_send()
        if m + ASLOTS < SIX:
            self.tell(self.acredit)

    def finish(self, m):
        self.store(m, 0, HALF, START).wait_recv()

    def squares(self, i):
        me, core, _ = coords()

        def copy(i):
            device = across(i - 1)[0] if i else me + 1 - 2 * core
            return pltpu.make_async_remote_copy(self.SQ.at[i], self.SQR.at[i], self.qs.at[i], self.qr.at[i], at(device), MESH)

        if i:
            copy(i - 1).wait()
            self.SQ[i] = self.SQ[i - 1] + self.SQR[i - 1]
        if i < 7:
            copy(i).start()


def tiles(body):
    @pl.loop(0, SIX)
    def _(i):
        body(i, TILE)

    body(jnp.int32(SIX), LANES)


def span(i, width):
    return pl.ds(pl.multiple_of(i * TILE, LANES), width)


def dot_t(a, b):
    return lax.dot_general(a, b, (((1,), (1,)), ((), ())), preferred_element_type=jnp.float32)


def go(copies, start):
    for c in copies:
        c.start() if start else c.wait()


def scale_of(wide):
    return lax.rsqrt(jnp.mean(wide * wide, -1, keepdims=START) + 1e-6)


def forward_kernel(x, dy, wg, wu, wd, a0_t, act0, gate, up, h1, a1_t, dy_t, act1, by_gate, by_up, XV, DY, AV, HV, TV, WS, WD, DT, ACT, ST, SB, sem, ws, ds, st, sb):
    def weights(layer, i, width, start):
        s = lax.rem(i, 2)
        go([pltpu.make_async_copy(w.at[layer, :, span(i, width)], WS.at[s, k, :, pl.ds(0, width)], ws.at[s, k]) for k, w in enumerate((wg, wu))], start)

    def downs(i, width, start):
        s = lax.rem(i, 2)
        go([pltpu.make_async_copy(wd.at[1, span(i, width), :], DT.at[s, pl.ds(0, width)], ds.at[s])], start)

    def saved(i, width, start):
        s = lax.rem(i, 2)
        go([pltpu.make_async_copy(ST.at[s, k, :, pl.ds(0, width)], o.at[:, span(i, width)], st.at[s, k]) for k, o in enumerate((gate, up))], start)

    def results(i, width, start):
        s = lax.rem(i, 2)
        go([pltpu.make_async_copy(SB.at[s, k, :, pl.ds(0, width)], o.at[:, span(i, width)], sb.at[s, k]) for k, o in enumerate((act1, by_gate, by_up))], start)

    def norm(states):
        for r in range(4):
            rows = slice(BLOCK * r, BLOCK * r + BLOCK)
            wide = states[rows].astype(jnp.float32)
            AV[rows] = (wide * scale_of(wide)).astype(jnp.bfloat16)

    def turn(a, t, i):
        TV[t, :, pl.ds(pl.multiple_of(i * LANES, LANES), LANES)] = a[pl.ds(pl.multiple_of(i * LANES, LANES), LANES), :].T

    x_in, dy_in, wd_in = (pltpu.make_async_copy(a, b, sem.at[k]) for k, (a, b) in enumerate(((x, XV), (dy, DY), (wd.at[0], WD))))
    x_in.start()
    weights(0, jnp.int32(0), TILE, START)
    weights(0, jnp.int32(1), TILE, START)
    wd_in.start()
    dy_in.start()
    x_in.wait()
    norm(XV)

    def first(i, width):
        s = lax.rem(i, 2)
        weights(0, i, width, WAIT)

        @pl.when(i >= 2)
        def _():
            saved(i - 2, TILE, WAIT)

        g = jnp.dot(AV[...], WS[s, 0, :, 0:width], preferred_element_type=jnp.float32)
        u = jnp.dot(AV[...], WS[s, 1, :, 0:width], preferred_element_type=jnp.float32)
        ST[s, 0, :, 0:width] = g
        ST[s, 1, :, 0:width] = u
        saved(i, width, START)
        ACT[:, span(i, width)] = (g * jax.nn.sigmoid(g) * u).astype(jnp.bfloat16)
        if width == TILE:
            turn(AV, 0, i)

            @pl.when(i < 4)
            def _():
                weights(0, i + 2, TILE, START)

            @pl.when(i == 4)
            def _():
                weights(0, jnp.int32(SIX), LANES, START)

    tiles(first)
    pl.loop(SIX, 8)(lambda i: turn(AV, 0, i))
    for i in range(2):
        weights(1, jnp.int32(i), TILE, START)
        downs(jnp.int32(i), TILE, START)
    outs = [pltpu.make_async_copy(TV.at[0], a0_t, sem.at[0]), pltpu.make_async_copy(ACT, act0, sem.at[3])]
    go(outs, START)
    wd_in.wait()
    dy_in.wait()

    @pl.loop(0, 4)
    def _(i):
        cols = pl.ds(pl.multiple_of(i * BLOCK, BLOCK), BLOCK)
        y = jnp.dot(ACT[...], WD[:, cols], preferred_element_type=jnp.float32)
        HV[:, cols] = XV[:, cols] + y.astype(jnp.bfloat16)
        for k in range(2):
            turn(DY, 1, 2 * i + k)

    later = [pltpu.make_async_copy(HV, h1, sem.at[1]), pltpu.make_async_copy(TV.at[1], dy_t, sem.at[2])]
    go(later, START)
    norm(HV)
    go(outs, WAIT)

    def second(i, width):
        s = lax.rem(i, 2)
        weights(1, i, width, WAIT)
        downs(i, width, WAIT)

        @pl.when(i >= 2)
        def _():
            results(i - 2, TILE, WAIT)

        g = jnp.dot(AV[...], WS[s, 0, :, 0:width], preferred_element_type=jnp.float32)
        u = jnp.dot(AV[...], WS[s, 1, :, 0:width], preferred_element_type=jnp.float32)
        d = dot_t(DY[...], DT[s, 0:width]).astype(jnp.bfloat16).astype(jnp.float32)
        sig = jax.nn.sigmoid(g)
        silu = g * sig
        SB[s, 0, :, 0:width] = (silu * u).astype(jnp.bfloat16)
        SB[s, 1, :, 0:width] = (d * u * (sig * (1 + g * (1 - sig)))).astype(jnp.bfloat16)
        SB[s, 2, :, 0:width] = (d * silu).astype(jnp.bfloat16)
        results(i, width, START)
        if width == TILE:
            turn(AV, 0, i)

            @pl.when(i < 4)
            def _():
                weights(1, i + 2, TILE, START)
                downs(i + 2, TILE, START)

            @pl.when(i == 4)
            def _():
                weights(1, jnp.int32(SIX), LANES, START)
                downs(jnp.int32(SIX), LANES, START)

    tiles(second)
    pl.loop(SIX, 8)(lambda i: turn(AV, 0, i))
    outs = [pltpu.make_async_copy(TV.at[0], a1_t, sem.at[0])]
    go(outs, START)
    saved(jnp.int32(5), TILE, WAIT)
    saved(jnp.int32(SIX), LANES, WAIT)
    results(jnp.int32(5), TILE, WAIT)
    results(jnp.int32(SIX), LANES, WAIT)
    go(outs + later, WAIT)


def forward(x, dy, wg, wu, wd):
    b, f, dma = jnp.bfloat16, jnp.float32, pltpu.SemaphoreType.DMA
    square, wide = (SIDE, SIDE), (SIDE, WIDE)
    vm = pltpu.VMEM
    outs = [(square, b), (wide, b), (wide, f), (wide, f), (square, b), (square, b), (square, b), (wide, b), (wide, b), (wide, b)]
    scratch = [vm(square, b)] * 2 + [vm(square, b)] * 2 + [vm((2, *square), b), vm((2, 2, SIDE, TILE), b), vm((WIDE, SIDE), b), vm((2, TILE, SIDE), b)]
    scratch += [vm(wide, b), vm((2, 2, SIDE, TILE), f), vm((2, 3, SIDE, TILE), b), dma((4,)), dma((2, 2)), dma((2,)), dma((2, 2)), dma((2, 3))]
    a0_t, act0, gate, up, h1, a1_t, dy_t, act1, by_gate1, by_up1 = pl.pallas_call(
        forward_kernel,
        out_shape=[jax.ShapeDtypeStruct(s, t) for s, t in outs],
        in_specs=[ANY] * 5,
        out_specs=[ANY] * 10,
        scratch_shapes=scratch,
        compiler_params=pltpu.CompilerParams(vmem_limit_bytes=62 * 2**20),
        name="forward",
    )(x, dy, wg, wu, wd)
    return dy_t, a1_t, a0_t, act1, by_gate1, by_up1, act0, wg, wu, wd, gate, up, h1, dy


SCRATCH = (
    ("X", (SIDE, WIDE), jnp.bfloat16),
    ("L", (2, SIDE, SIDE), jnp.bfloat16),
    ("OUT", (HALF, LANES), jnp.bfloat16),
    ("RP", (HALF, LANES), jnp.bfloat16),
    ("O", (SLOTS, 9600, LANES), jnp.bfloat16),
    ("R", (SLOTS, HALF, LANES), jnp.bfloat16),
    ("F", (SLOTS, QUARTER, LANES), jnp.float32),
    ("A", (ASLOTS, HALF, LANES), jnp.bfloat16),
    ("SQ", (8, 8, LANES), jnp.float32),
    ("SQR", (7, 8, LANES), jnp.float32),
    ("DA", (SIDE, SIDE), jnp.float32),
    ("WT", (2, SIDE, 640), jnp.bfloat16),
    ("BY", (SIDE, SIDE), jnp.bfloat16),
    ("GU", (2, 2, SIDE, BLOCK), jnp.float32),
    ("WD", (2, BLOCK, SIDE), jnp.bfloat16),
    ("DS", (2, SIDE, BLOCK), jnp.bfloat16),
)
SEMAPHORES = (
    ("ss", (SLOTS, SIX)), ("rs", (SLOTS, SIX, SIX)), ("ps", (SIX, 2)), ("pr", (SIX, 2)), ("gs", (ASLOTS, SIX)), ("gr", (ASLOTS, SIX, SIX)),
    ("gl", (ASLOTS,)), ("ds", (ASLOTS,)), ("dr", (SIX,)), ("qs", (7,)), ("qr", (7,)), ("xs", (SIX,)), ("ls", (2,)),
    ("wts", (2,)), ("hs", (2,)), ("gus", (2, 3)), ("dus", (2,)),
)


def gradients_kernel(*refs, order):
    dy_t, a1_t, a0_t, act1, by_gate1, by_up1, act0, w_gate, w_up, w_down, gate, up, h1, dy = refs[:14]
    g, factor, by_up0 = refs[14:17]
    r = dict(zip([s[0] for s in SCRATCH + SEMAPHORES] + ["credit", "acredit", "pcredit"], refs[17:], strict=START))
    X, L, OUT, RP, O, F, DA, WT, BY, GU, WD, DS = (r[n] for n in ("X", "L", "OUT", "RP", "O", "F", "DA", "WT", "BY", "GU", "WD", "DS"))
    comm = Comm(r, g)
    me, core, _ = coords()
    partner = me + 1 - 2 * core
    left_of = (0, 1, 1, 0, 1, 1)
    rights = (act1, by_up1, by_gate1, act0, None, by_up0)

    def left(a, i):
        return pltpu.make_async_copy(a, L.at[i], r["ls"].at[i])

    def right(m, j, slabs):
        cols = pl.ds(al(j * TILE, LANES), LANES * slabs)
        return pltpu.make_async_copy(rights[m].at[:, cols], X.at[:, cols], r["xs"].at[j])

    def row_tile(which, j):
        cols = pl.ds(al(j * TILE, LANES), 640)
        slot = lax.rem(j, 2)
        return pltpu.make_async_copy((w_up, w_gate)[which].at[1, :, cols], WT.at[slot], r["wts"].at[slot])

    def hidden(t, width, start):
        s, cols = lax.rem(t, 2), pl.ds(al(t * BLOCK, LANES), width)
        copies = [pltpu.make_async_copy(a.at[:, cols], GU.at[s, k, :, pl.ds(0, width)], r["gus"].at[s, k]) for k, a in enumerate((gate, up))]
        go(copies + [pltpu.make_async_copy(w_down.at[0, cols, :], WD.at[s, pl.ds(0, width)], r["gus"].at[s, 2])], start)

    def put(t, width, start):
        s, cols = lax.rem(t, 2), pl.ds(al(t * BLOCK, LANES), width)
        go([pltpu.make_async_copy(DS.at[s, :, pl.ds(0, width)], by_up0.at[:, cols], r["dus"].at[s])], start)

    left(dy_t, 0).start()
    colors(lambda j, slabs: right(0, j, slabs).start())
    left(a1_t, 1).start()
    dy_in = pltpu.make_async_copy(dy, BY, r["hs"].at[0])
    h_in = pltpu.make_async_copy(h1, L.at[0], r["hs"].at[1])
    dy_in.start()
    row_tile(0, 0).start()
    hidden(0, BLOCK, START)
    hidden(1, BLOCK, START)
    comm.tables()
    barrier = pltpu.get_barrier_semaphore()
    for d in range(SIX):
        pl.semaphore_signal(barrier, inc=1, device_id=at(across(d)[0]), device_id_type=MESH)
    pl.semaphore_signal(barrier, inc=1, device_id=at(partner), device_id_type=MESH)
    r["SQ"][0] = jnp.zeros((8, LANES), jnp.float32)
    for b in range(4):
        DA[BLOCK * b : BLOCK * b + BLOCK] = jnp.zeros((BLOCK, SIDE), jnp.float32)
    pl.semaphore_wait(barrier, 7)

    def dot(m, row, rows, j, slabs):
        return jnp.dot(
            L[left_of[m], pl.ds(al(row, BLOCK), rows), :],
            X[:, pl.ds(al(j * TILE, TILE), LANES * slabs)],
            preferred_element_type=jnp.float32,
        )

    def theirs(m):
        if m == 0:
            left(dy_t, 0).wait()
        if m == 1:
            left(a1_t, 1).wait()
        if m == 4:
            left(a0_t, 1).wait()
        if m:
            pl.semaphore_wait(r["pcredit"], 1)

        def body(j, slabs):
            n = TILE * slabs
            if m != 4:
                right(m, j, slabs).wait()
            if m:
                for h in range(2):
                    comm.pair(m, j, n, h, partner).wait_send()
            res = dot(m, (1 - core) * TILE, TILE, j, slabs).astype(jnp.bfloat16)
            for h in range(2):
                for s in range(slabs):
                    OUT[pl.ds(al(h * QUARTER + j * SIDE + s * BLOCK), BLOCK)] = res[h * BLOCK : h * BLOCK + BLOCK, s * LANES : s * LANES + LANES]
                comm.pair(m, j, n, h, partner).start()

        colors(body)

    def ours(m):
        slot = m % SLOTS
        if m >= SLOTS:
            for d in range(SIX):
                pl.semaphore_wait(r["credit"].at[d], 1)

        @pl.loop(0, 2)
        def _(stays):
            def body(j, slabs):
                n = TILE * slabs
                device, side = comm.other(m, j, 1), comm.side(m, j, 1)
                h = stays * side + (1 - stays) * (1 - side)
                comm.pair(m, j, n, h, partner).wait_recv()
                res = dot(m, core * TILE + h * BLOCK, BLOCK, j, slabs)

                def total(s):
                    return res[:, s * LANES : s * LANES + LANES] + RP[pl.ds(al(h * QUARTER + j * SIDE + s * BLOCK), BLOCK)].astype(jnp.float32)

                @pl.when(stays == 0)
                def _():
                    for s in range(slabs):
                        O[slot, pl.ds(al(comm.sent(j, n, 1) + s * BLOCK), BLOCK)] = total(s).astype(jnp.bfloat16)
                    comm.rdma(m, j, n, 1, device).start()

                @pl.when(stays == 1)
                def _():
                    for s in range(slabs):
                        F[slot, pl.ds(al(j * SIDE + s * BLOCK), BLOCK)] = total(s)
                    if m in (0, 4):
                        right(m + 1, j, slabs).start()

            colors(body)

        if m < 5:
            pl.semaphore_signal(r["pcredit"], inc=1, device_id=at(partner), device_id_type=MESH)
        if m == 0:
            h_in.start()
        if m == 2:
            left(a0_t, 1).start()

    def by_normed(i):
        which, part = divmod(i, 3)

        def body(j, slabs):
            cols = pl.ds(al(j * TILE, LANES), LANES * slabs)
            row_tile(which, j).wait()
            if isinstance(j, int):
                if which == 0:
                    row_tile(1, 0).start()
            else:
                row_tile(which, j + 1).start()
            for half in range(2):
                rows = slice(TILE * half, TILE * half + TILE)
                part_of = dot_t(X[rows, cols], WT[lax.rem(j, 2), :, 0 : LANES * slabs])
                DA[rows] += part_of
            right(2 + which, j, slabs).start()

        if part == 2:
            body(5, 5)
        else:

            @pl.loop(3 * part, 3 + 2 * part)
            def _(j):
                body(j, 4)

    def normed_back():
        dy_in.wait()
        h_in.wait()

        @pl.loop(0, 8)
        def _(b):
            rows = pl.ds(al(b * LANES, LANES), LANES)
            wide = L[0, rows].astype(jnp.float32)
            scale = scale_of(wide)
            d = DA[rows].astype(jnp.bfloat16).astype(jnp.float32)
            through = d * scale - wide * (scale * scale * scale * jnp.mean(d * wide, -1, keepdims=START))
            BY[rows] = BY[rows] + through.astype(jnp.bfloat16)

        @pl.loop(0, 8)
        def _(b):
            rows = pl.ds(al(b * LANES, LANES), LANES)
            L[0, :, rows] = BY[rows].T

    def by_hidden(i):
        def body(t, width):
            s = lax.rem(t, 2)
            hidden(t, width, WAIT)

            @pl.when(t >= 2)
            def _():
                put(t - 2, BLOCK, WAIT)

            @pl.loop(0, 2)
            def _(half):
                rows = pl.ds(al(half * TILE, TILE), TILE)
                d = dot_t(BY[rows], WD[s, 0:width]).astype(jnp.bfloat16).astype(jnp.float32)
                gt = GU[s, 0, rows, 0:width]
                sig = jax.nn.sigmoid(gt)
                X[rows, pl.ds(al(t * BLOCK, LANES), width)] = (d * GU[s, 1, rows, 0:width] * (sig * (1 + gt * (1 - sig)))).astype(jnp.bfloat16)
                DS[s, rows, 0:width] = (d * (gt * sig)).astype(jnp.bfloat16)

            put(t, width, START)
            if width == BLOCK:

                @pl.when(t < 10)
                def _():
                    hidden(t + 2, BLOCK, START)

                @pl.when(t == 10)
                def _():
                    hidden(12, LANES, START)

        if i < 3:

            @pl.loop(4 * i, 4 * i + 4)
            def _(t):
                body(t, BLOCK)

        else:
            body(jnp.int32(12), LANES)
            put(11, BLOCK, WAIT)
            put(12, LANES, WAIT)

    def run(kind, m, k):
        if kind == "theirs":
            theirs(m)
        elif kind == "ours":
            ours(m)
        elif kind == "normed":
            by_normed(m)
        elif kind == "back_normed":
            normed_back()
        elif kind == "hidden":
            by_hidden(m)
        elif kind == "add":
            comm.add(m, k)
        elif kind == "back":
            comm.back(m, k)
        elif kind == "free":
            comm.free(m)
        elif kind == "sq":
            comm.squares(m)

    for item in order:
        if SCOPES:
            with jax.named_scope("_".join(str(i) for i in item)):
                run(*item)
        else:
            run(*item)
    for m in range(SIX):
        comm.finish(m)

    def last(j, slabs):
        for h in range(2):
            comm.pair(5, j, TILE * slabs, h, partner).wait_send()

    colors(last)
    total = jnp.sum(jnp.sum(r["SQ"][7], 1, keepdims=START), 0, keepdims=START)
    count = SIX * ROWS * LANES
    factor[...] = jnp.broadcast_to(jnp.minimum(1.0, 0.5 * lax.rsqrt(total / count + 1e-30)), (8, LANES))


def summed_gradients(order, *args):
    dma = pltpu.SemaphoreType.DMA
    regular = pltpu.SemaphoreType.REGULAR
    return pl.pallas_call(
        functools.partial(gradients_kernel, order=order),
        out_shape=(jax.ShapeDtypeStruct((SIX * ROWS, LANES), jnp.bfloat16), jax.ShapeDtypeStruct((8, LANES), jnp.float32), jax.ShapeDtypeStruct((SIDE, WIDE), jnp.bfloat16)),
        in_specs=[ANY] * 14,
        out_specs=[ANY, pl.BlockSpec(memory_space=pltpu.VMEM), ANY],
        scratch_shapes=[pltpu.VMEM(shape, t) for _, shape, t in SCRATCH] + [dma(shape) for _, shape in SEMAPHORES] + [regular((SIX,)), regular((SIX,)), regular],
        compiler_params=pltpu.CompilerParams(collective_id=0, has_side_effects=START, vmem_limit_bytes=67043328),
        name="gradients",
    )(*args)


CHOICES = (
    293090303584272896, 439771127150294081, 586143053359101962, 840934915364247578,
    845761179014392182, 114748407,
)


def steps():
    compute = []
    for m in range(SIX):
        compute += [(kind, m, -1) for kind in ("theirs", "ours")]
        if m in (1, 2):
            compute += [("normed", 3 * m - 3 + i, -1) for i in range(3)]
        if m == 2:
            compute.append(("back_normed", 0, -1))
        if m == 3:
            compute += [("hidden", i, -1) for i in range(4)]
    chains = [compute]
    for m in range(SIX):
        chains.append([("add", m, k) for k in range(1, 7)] + [("back", m, k) for k in range(5, -1, -1)] + [("free", m, 0)])
    chains.append([("sq", i, 0) for i in range(8)])
    chains = [iter(chain) for chain in chains]
    count = 109
    return [next(chains[CHOICES[i // 20] >> (3 * (i % 20)) & 7]) for i in range(count)]


ROWS_A = 64
DEEP = 4


def adam_kernel(factor, g, *refs):
    ins, outs = (refs[0:3], refs[3:SIX], refs[SIX:9]), (refs[9:12], refs[12:15], refs[15:18])
    gf, gt, *rest = refs[18:]
    flat_in, turned_in, flat_out, turned_out, got, put = rest[0:3], rest[3:SIX], rest[SIX:9], rest[9:12], rest[12], rest[13]
    per = SIDE // ROWS_A
    flat, tiles = 4 * per, 4 * per + 50

    def pieces(i, act):
        for n in range(3):
            first, count = (0, per) if n == 0 else (2 * per, per) if n == 1 else (4 * per, 25)

            @pl.when((i >= first) & (i < first + 2 * count))
            def _():
                layer, t = lax.div(i - first, count), lax.rem(i - first, count)
                chunk = (layer * (2 - n) + (1 - layer) * (4, 5, 3)[n]) * 4
                rows = LANES if n == 2 else ROWS_A
                place = (layer, pl.ds(pl.multiple_of(t * rows, rows), rows))
                if n == 2:
                    act(n, place, g.at[pl.ds(chunk, 4), t])
                else:
                    part = BLOCK // ROWS_A
                    act(n, place, g.at[chunk + lax.div(t, part), :, pl.ds(pl.multiple_of(lax.rem(t, part) * ROWS_A, ROWS_A), ROWS_A)])

    def load(i, start):
        slot = lax.rem(i, DEEP)

        def act(n, place, grads):
            copies = [pltpu.make_async_copy(grads, (gt if n == 2 else gf).at[slot], got.at[slot, 3])]
            for k in range(3):
                buffer = (turned_in if n == 2 else flat_in)[k]
                copies.append(pltpu.make_async_copy(ins[k][n].at[place], buffer.at[slot], got.at[slot, k]))
            for c in copies:
                c.start() if start else c.wait()

        pieces(i, act)

    def store(i, start):
        slot = lax.rem(i, DEEP)

        def act(n, place, grads):
            for k in range(3):
                buffer = (turned_out if n == 2 else flat_out)[k]
                c = pltpu.make_async_copy(buffer.at[slot], outs[k][n].at[place], put.at[slot, k])
                c.start() if start else c.wait()

        pieces(i, act)

    def compute(i, turned):
        slot = lax.rem(i, DEEP)
        w, m, v = turned_in if turned else flat_in
        w_out, m_out, v_out = turned_out if turned else flat_out
        f = factor[0:1, 0:1] if turned else factor[0:1, :]

        def part(s):
            if turned:
                piece = gt[slot, s].astype(jnp.float32).T
                where = (slot, slice(None), pl.ds(pl.multiple_of(BLOCK * s, BLOCK), BLOCK))
            else:
                piece = gf[slot, s].astype(jnp.float32)
                where = (slot, slice(None), pl.ds(pl.multiple_of(LANES * s, LANES), LANES))
            piece = piece * f
            new_m = 0.9 * m[where] + 0.1 * piece
            new_v = 0.95 * v[where] + 0.05 * piece * piece
            wide = w[where].astype(jnp.float32)
            step = new_m * lax.rsqrt(new_v + 1e-8) + 0.1 * wide
            m_out[where] = new_m
            v_out[where] = new_v
            w_out[where] = (wide - 0.02 * step).astype(jnp.bfloat16)

        if turned:
            pl.loop(0, 4)(part)
        else:

            @pl.loop(0, 5)
            def _(i):
                for s in range(5):
                    part(5 * i + s)

    @pl.loop(0, DEEP - 1)
    def _(i):
        load(i, START)


    @pl.loop(0, tiles)
    def _(i):
        @pl.when(i + DEEP - 1 < tiles)
        def _():
            load(i + DEEP - 1, START)

        load(i, WAIT)

        @pl.when(i >= DEEP)
        def _():
            store(i - DEEP, WAIT)

        @pl.when(i < flat)
        def _():
            compute(i, WAIT)

        @pl.when(i >= flat)
        def _():
            compute(i, START)

        store(i, START)

    @pl.loop(tiles - DEEP, tiles)
    def _(i):
        store(i, WAIT)


def adam(factor, g, weights, m, v):
    arrays = (*weights, *m, *v)
    flat, turned = (DEEP, ROWS_A, WIDE), (DEEP, LANES, SIDE)
    types = (jnp.bfloat16, jnp.float32, jnp.float32)
    return pl.pallas_call(
        adam_kernel,
        out_shape=tuple(jax.ShapeDtypeStruct(a.shape, a.dtype) for a in arrays),
        in_specs=[pl.BlockSpec(memory_space=pltpu.VMEM), ANY] + [ANY] * 9,
        out_specs=(ANY,) * 9,
        scratch_shapes=[pltpu.VMEM((DEEP, 25, ROWS_A, LANES), jnp.bfloat16), pltpu.VMEM((DEEP, 4, BLOCK, LANES), jnp.bfloat16)]
        + [pltpu.VMEM(shape, t) for _ in range(2) for shape in (flat, turned) for t in types]
        + [pltpu.SemaphoreType.DMA((DEEP, 4)), pltpu.SemaphoreType.DMA((DEEP, 3))],
        compiler_params=pltpu.CompilerParams(vmem_limit_bytes=60 * 2**20),
        name="adam",
    )(factor, g.reshape(24, 25, BLOCK, LANES), *arrays)


def solution(mesh):
    order = steps()

    def step(x, dy, *arrays):
        weights, m, v = (arrays[i : i + 3] for i in (0, 3, SIX))
        g, factor, _ = summed_gradients(order, *forward(x[0], dy[0], *weights))
        return tuple(adam(factor, g, weights, m, v))

    return jax.shard_map(
        step,
        mesh=mesh,
        in_specs=(P(("rep", "dp"), None, None),) * 2 + (P(None, None, None),) * 9,
        out_specs=(P("rep", None, None),) * 9,
        check_vma=WAIT,
    )
```

```python
import functools

import jax
import jax.numpy as jnp
from jax import lax
from jax.experimental import pallas as pl
from jax.experimental.pallas import tpu as pltpu
from jax.sharding import PartitionSpec as P

LANES, BLOCK, TILE, SIDE, WIDE, SIX = 128, 256, 512, 1024, 3200, 6
START, WAIT = True, False
MESH = pl.DeviceIdType.MESH
ANY = pl.BlockSpec(memory_space=pl.ANY)
ROWS, HALF, QUARTER = 25600, 12800, 6400
STEPS = SIX
SLOTS, ASLOTS = 2, 3
SCOPES = WAIT


def coords():
    me = lax.axis_index("dp")
    return me, lax.rem(me, 2), (lax.div(me, 32), lax.rem(lax.div(me, 8), 4), lax.rem(lax.div(me, 2), 4))


def across(d):
    me, _, xyz = coords()
    c, stride = xyz[d // 2], (32, 8, 2)[d // 2]
    if d % 2:
        return me + (3 - 2 * c) * stride, lax.div(c, 2)
    return me + (1 - 2 * lax.rem(c, 2)) * stride, lax.rem(lax.div(c + 1, 2), 2)


def al(v, n=8):
    return pl.multiple_of(v, n)


def colors(body):
    @pl.loop(0, 5)
    def _(j):
        body(j, 4)

    body(5, 5)


def at(device):
    return {"dp": device}


class Comm:
    def __init__(self, refs, g):
        self.__dict__.update(refs)
        self.g = g

    def tables(self):
        pairs = [across(d) for d in range(SIX)]
        self.others, self.sides = [o for o, _ in pairs], [side for _, side in pairs]

    def pick(self, values, m, j, k):
        d = j + (m + k - 1) % SIX
        if isinstance(d, int):
            return values[d % SIX]
        d = lax.rem(d, SIX)
        value = values[0]
        for i in range(1, SIX):
            value = jnp.where(d == i, values[i], value)
        return value

    def other(self, m, j, k):
        return self.pick(self.others, m, j, k)

    def side(self, m, j, k):
        return self.pick(self.sides, m, j, k)

    def sent(self, j, n, k):
        return j * 1536 + (0 if k % 2 else n // 2)

    def rdma(self, m, j, n, k, device):
        s, h = m % SLOTS, n >> k
        rows = pl.ds(al(j * 2048 + (n - (n >> (k - 1)))), h)
        mine = pl.ds(al(self.sent(j, n, k)), h)
        return pltpu.make_async_remote_copy(self.O.at[s, mine], self.R.at[s, rows], self.ss.at[s, j], self.rs.at[s, j, k - 1], at(device), MESH)

    def pair(self, m, j, n, h, device):
        rows = pl.ds(al(h * QUARTER + j * SIDE), n // 2)
        return pltpu.make_async_remote_copy(self.OUT.at[rows], self.RP.at[rows], self.ps.at[j, h], self.pr.at[j, h], at(device), MESH)

    def add(self, m, k):
        s = m % SLOTS

        def body(j, slabs):
            n = TILE * slabs
            got = self.rdma(m, j, n, k, self.other(m, j, k))
            got.wait()
            base, fb = j * 2048 + (n - (n >> (k - 1))), j * SIDE
            if k < STEPS:
                h = n >> (k + 1)
                device, side = self.other(m, j, k + 1), self.side(m, j, k + 1)
                step = min(h, 32 * slabs)

                @pl.loop(0, h // step)
                def _(i):
                    o = (1 - side) * h + i * step
                    total = self.F[s, pl.ds(al(fb + o), step)] + self.R[s, pl.ds(al(base + o), step)].astype(jnp.float32)
                    self.O[s, pl.ds(al(self.sent(j, n, k + 1) + i * step), step)] = total.astype(jnp.bfloat16)

                self.rdma(m, j, n, k + 1, device).start()

                @pl.loop(0, h // step)
                def _(i):
                    o = side * h + i * step
                    total = self.F[s, pl.ds(al(fb + o), step)] + self.R[s, pl.ds(al(base + o), step)].astype(jnp.float32)
                    self.F[s, pl.ds(al(fb + i * step), step)] = total

            else:
                h = n >> k
                total = self.F[s, pl.ds(al(fb), h)] + self.R[s, pl.ds(al(base), h)].astype(jnp.float32)
                total = total.astype(jnp.bfloat16)
                self.A[m % ASLOTS, pl.ds(al(self.row(m, j, n, k)), h)] = total
                self.gather(m, j, n, k).start()
                wide = total.astype(jnp.float32)
                self.SQ[0] += jnp.sum((wide * wide).reshape(h // 8, 8, LANES), 0)

        if k == STEPS and m >= ASLOTS:
            for d in range(SIX):
                pl.semaphore_wait(self.acredit.at[d], 1)
        colors(body)
        if k == STEPS and m + SLOTS < SIX:
            self.tell(self.credit)

    def tell(self, credit):
        for d in range(SIX):
            pl.semaphore_signal(credit.at[d], inc=1, device_id=at(across(d)[0]), device_id_type=MESH)

    def row(self, m, j, n, k, flip=WAIT):
        row = j * SIDE
        for i in range(1, k + 1):
            side = self.side(m, j, i)
            if flip and i == k:
                side = 1 - side
            row = row + side * (QUARTER if i == 1 else n >> i)
        return row

    def gather(self, m, j, n, k):
        a = m % ASLOTS
        part = self.A.at[a, pl.ds(al(self.row(m, j, n, k)), n >> k)]
        return pltpu.make_async_remote_copy(part, part, self.gs.at[a, j], self.gr.at[a, j, k - 1], at(self.other(m, j, k)), MESH)

    def store(self, m, row, rows, away):
        me, core, _ = coords()
        a = m % ASLOTS
        part = self.A.at[a, pl.ds(al(row), rows)]
        to = self.g.at[pl.ds(al(m * ROWS + core * HALF + row), rows)]
        if not away:
            return pltpu.make_async_copy(part, to, self.gl.at[a])
        return pltpu.make_async_remote_copy(part, to, self.ds.at[a], self.dr.at[m], at(me + 1 - 2 * core), MESH)

    def back(self, m, k):
        def body(j, slabs):
            n = TILE * slabs
            self.gather(m, j, n, k + 1).wait()
            if k:
                self.gather(m, j, n, k).start()
            if k <= 2:
                half = 2 if k else 1
                row = self.row(m, j, n, half, k < 2)
                for away in (WAIT, START):
                    self.store(m, row, n >> half, away).start()

        colors(body)

    def free(self, m):
        self.store(m, 0, HALF, WAIT).wait()
        self.store(m, 0, HALF, START).wait_send()
        if m + ASLOTS < SIX:
            self.tell(self.acredit)

    def finish(self, m):
        self.store(m, 0, HALF, START).wait_recv()

    def squares(self, i):
        me, core, _ = coords()

        def copy(i):
            device = across(i - 1)[0] if i else me + 1 - 2 * core
            return pltpu.make_async_remote_copy(self.SQ.at[i], self.SQR.at[i], self.qs.at[i], self.qr.at[i], at(device), MESH)

        if i:
            copy(i - 1).wait()
            self.SQ[i] = self.SQ[i - 1] + self.SQR[i - 1]
        if i < 7:
            copy(i).start()


def tiles(body):
    @pl.loop(0, SIX)
    def _(i):
        body(i, TILE)

    body(jnp.int32(SIX), LANES)


def span(i, width):
    return pl.ds(pl.multiple_of(i * TILE, LANES), width)


def dot_t(a, b):
    return lax.dot_general(a, b, (((1,), (1,)), ((), ())), preferred_element_type=jnp.float32)


def go(copies, start):
    for c in copies:
        c.start() if start else c.wait()


def scale_of(wide):
    return lax.rsqrt(jnp.mean(wide * wide, -1, keepdims=START) + 1e-6)


def forward_kernel(x, dy, wg, wu, wd, a0_t, act0, gate, up, h1, a1_t, dy_t, act1, by_gate, by_up, XV, DY, AV, HV, TV, WS, WD, DT, ACT, ST, SB, sem, ws, ds, st, sb):
    def weights(layer, i, width, start):
        s = lax.rem(i, 2)
        go([pltpu.make_async_copy(w.at[layer, :, span(i, width)], WS.at[s, k, :, pl.ds(0, width)], ws.at[s, k]) for k, w in enumerate((wg, wu))], start)

    def downs(i, width, start):
        s = lax.rem(i, 2)
        go([pltpu.make_async_copy(wd.at[1, span(i, width), :], DT.at[s, pl.ds(0, width)], ds.at[s])], start)

    def saved(i, width, start):
        s = lax.rem(i, 2)
        go([pltpu.make_async_copy(ST.at[s, k, :, pl.ds(0, width)], o.at[:, span(i, width)], st.at[s, k]) for k, o in enumerate((gate, up))], start)

    def results(i, width, start):
        s = lax.rem(i, 2)
        go([pltpu.make_async_copy(SB.at[s, k, :, pl.ds(0, width)], o.at[:, span(i, width)], sb.at[s, k]) for k, o in enumerate((act1, by_gate, by_up))], start)

    def norm(states):
        for r in range(4):
            rows = slice(BLOCK * r, BLOCK * r + BLOCK)
            wide = states[rows].astype(jnp.float32)
            AV[rows] = (wide * scale_of(wide)).astype(jnp.bfloat16)

    def turn(a, t, i):
        TV[t, :, pl.ds(pl.multiple_of(i * LANES, LANES), LANES)] = a[pl.ds(pl.multiple_of(i * LANES, LANES), LANES), :].T

    x_in, dy_in, wd_in = (pltpu.make_async_copy(a, b, sem.at[k]) for k, (a, b) in enumerate(((x, XV), (dy, DY), (wd.at[0], WD))))
    x_in.start()
    weights(0, jnp.int32(0), TILE, START)
    weights(0, jnp.int32(1), TILE, START)
    wd_in.start()
    dy_in.start()
    x_in.wait()
    norm(XV)

    def first(i, width):
        s = lax.rem(i, 2)
        weights(0, i, width, WAIT)

        @pl.when(i >= 2)
        def _():
            saved(i - 2, TILE, WAIT)

        g = jnp.dot(AV[...], WS[s, 0, :, 0:width], preferred_element_type=jnp.float32)
        u = jnp.dot(AV[...], WS[s, 1, :, 0:width], preferred_element_type=jnp.float32)
        ST[s, 0, :, 0:width] = g
        ST[s, 1, :, 0:width] = u
        saved(i, width, START)
        ACT[:, span(i, width)] = (g * jax.nn.sigmoid(g) * u).astype(jnp.bfloat16)
        if width == TILE:
            turn(AV, 0, i)

            @pl.when(i < 4)
            def _():
                weights(0, i + 2, TILE, START)

            @pl.when(i == 4)
            def _():
                weights(0, jnp.int32(SIX), LANES, START)

    tiles(first)
    pl.loop(SIX, 8)(lambda i: turn(AV, 0, i))
    for i in range(2):
        weights(1, jnp.int32(i), TILE, START)
        downs(jnp.int32(i), TILE, START)
    outs = [pltpu.make_async_copy(TV.at[0], a0_t, sem.at[0]), pltpu.make_async_copy(ACT, act0, sem.at[3])]
    go(outs, START)
    wd_in.wait()
    dy_in.wait()

    @pl.loop(0, 4)
    def _(i):
        cols = pl.ds(pl.multiple_of(i * BLOCK, BLOCK), BLOCK)
        y = jnp.dot(ACT[...], WD[:, cols], preferred_element_type=jnp.float32)
        HV[:, cols] = XV[:, cols] + y.astype(jnp.bfloat16)
        for k in range(2):
            turn(DY, 1, 2 * i + k)

    later = [pltpu.make_async_copy(HV, h1, sem.at[1]), pltpu.make_async_copy(TV.at[1], dy_t, sem.at[2])]
    go(later, START)
    norm(HV)
    go(outs, WAIT)

    def second(i, width):
        s = lax.rem(i, 2)
        weights(1, i, width, WAIT)
        downs(i, width, WAIT)

        @pl.when(i >= 2)
        def _():
            results(i - 2, TILE, WAIT)

        g = jnp.dot(AV[...], WS[s, 0, :, 0:width], preferred_element_type=jnp.float32)
        u = jnp.dot(AV[...], WS[s, 1, :, 0:width], preferred_element_type=jnp.float32)
        d = dot_t(DY[...], DT[s, 0:width]).astype(jnp.bfloat16).astype(jnp.float32)
        sig = jax.nn.sigmoid(g)
        silu = g * sig
        SB[s, 0, :, 0:width] = (silu * u).astype(jnp.bfloat16)
        SB[s, 1, :, 0:width] = (d * u * (sig * (1 + g * (1 - sig)))).astype(jnp.bfloat16)
        SB[s, 2, :, 0:width] = (d * silu).astype(jnp.bfloat16)
        results(i, width, START)
        if width == TILE:
            turn(AV, 0, i)

            @pl.when(i < 4)
            def _():
                weights(1, i + 2, TILE, START)
                downs(i + 2, TILE, START)

            @pl.when(i == 4)
            def _():
                weights(1, jnp.int32(SIX), LANES, START)
                downs(jnp.int32(SIX), LANES, START)

    tiles(second)
    pl.loop(SIX, 8)(lambda i: turn(AV, 0, i))
    outs = [pltpu.make_async_copy(TV.at[0], a1_t, sem.at[0])]
    go(outs, START)
    saved(jnp.int32(5), TILE, WAIT)
    saved(jnp.int32(SIX), LANES, WAIT)
    results(jnp.int32(5), TILE, WAIT)
    results(jnp.int32(SIX), LANES, WAIT)
    go(outs + later, WAIT)


def forward(x, dy, wg, wu, wd):
    b, f, dma = jnp.bfloat16, jnp.float32, pltpu.SemaphoreType.DMA
    square, wide = (SIDE, SIDE), (SIDE, WIDE)
    vm = pltpu.VMEM
    outs = [(square, b), (wide, b), (wide, f), (wide, f), (square, b), (square, b), (square, b), (wide, b), (wide, b), (wide, b)]
    scratch = [vm(square, b)] * 2 + [vm(square, b)] * 2 + [vm((2, *square), b), vm((2, 2, SIDE, TILE), b), vm((WIDE, SIDE), b), vm((2, TILE, SIDE), b)]
    scratch += [vm(wide, b), vm((2, 2, SIDE, TILE), f), vm((2, 3, SIDE, TILE), b), dma((4,)), dma((2, 2)), dma((2,)), dma((2, 2)), dma((2, 3))]
    a0_t, act0, gate, up, h1, a1_t, dy_t, act1, by_gate1, by_up1 = pl.pallas_call(
        forward_kernel,
        out_shape=[jax.ShapeDtypeStruct(s, t) for s, t in outs],
        in_specs=[ANY] * 5,
        out_specs=[ANY] * 10,
        scratch_shapes=scratch,
        compiler_params=pltpu.CompilerParams(vmem_limit_bytes=62 * 2**20),
        name="forward",
    )(x, dy, wg, wu, wd)
    return dy_t, a1_t, a0_t, act1, by_gate1, by_up1, act0, wg, wu, wd, gate, up, h1, dy


SCRATCH = (
    ("X", (SIDE, WIDE), jnp.bfloat16),
    ("L", (2, SIDE, SIDE), jnp.bfloat16),
    ("OUT", (HALF, LANES), jnp.bfloat16),
    ("RP", (HALF, LANES), jnp.bfloat16),
    ("O", (SLOTS, 9600, LANES), jnp.bfloat16),
    ("R", (SLOTS, HALF, LANES), jnp.bfloat16),
    ("F", (SLOTS, QUARTER, LANES), jnp.float32),
    ("A", (ASLOTS, HALF, LANES), jnp.bfloat16),
    ("SQ", (8, 8, LANES), jnp.float32),
    ("SQR", (7, 8, LANES), jnp.float32),
    ("DA", (SIDE, SIDE), jnp.float32),
    ("WT", (2, SIDE, 640), jnp.bfloat16),
    ("BY", (SIDE, SIDE), jnp.bfloat16),
    ("GU", (2, 2, SIDE, BLOCK), jnp.float32),
    ("WD", (2, BLOCK, SIDE), jnp.bfloat16),
    ("DS", (2, SIDE, BLOCK), jnp.bfloat16),
)
SEMAPHORES = (
    ("ss", (SLOTS, SIX)), ("rs", (SLOTS, SIX, SIX)), ("ps", (SIX, 2)), ("pr", (SIX, 2)), ("gs", (ASLOTS, SIX)), ("gr", (ASLOTS, SIX, SIX)),
    ("gl", (ASLOTS,)), ("ds", (ASLOTS,)), ("dr", (SIX,)), ("qs", (7,)), ("qr", (7,)), ("xs", (SIX,)), ("ls", (2,)),
    ("wts", (2,)), ("hs", (2,)), ("gus", (2, 3)), ("dus", (2,)),
)


def gradients_kernel(*refs, order):
    dy_t, a1_t, a0_t, act1, by_gate1, by_up1, act0, w_gate, w_up, w_down, gate, up, h1, dy = refs[:14]
    g, factor, by_up0 = refs[14:17]
    r = dict(zip([s[0] for s in SCRATCH + SEMAPHORES] + ["credit", "acredit", "pcredit"], refs[17:], strict=START))
    X, L, OUT, RP, O, F, DA, WT, BY, GU, WD, DS = (r[n] for n in ("X", "L", "OUT", "RP", "O", "F", "DA", "WT", "BY", "GU", "WD", "DS"))
    comm = Comm(r, g)
    me, core, _ = coords()
    partner = me + 1 - 2 * core
    left_of = (0, 1, 1, 0, 1, 1)
    rights = (act1, by_up1, by_gate1, act0, None, by_up0)

    def left(a, i):
        return pltpu.make_async_copy(a, L.at[i], r["ls"].at[i])

    def right(m, j, slabs):
        cols = pl.ds(al(j * TILE, LANES), LANES * slabs)
        return pltpu.make_async_copy(rights[m].at[:, cols], X.at[:, cols], r["xs"].at[j])

    def row_tile(which, j):
        cols = pl.ds(al(j * TILE, LANES), 640)
        slot = lax.rem(j, 2)
        return pltpu.make_async_copy((w_up, w_gate)[which].at[1, :, cols], WT.at[slot], r["wts"].at[slot])

    def hidden(t, width, start):
        s, cols = lax.rem(t, 2), pl.ds(al(t * BLOCK, LANES), width)
        copies = [pltpu.make_async_copy(a.at[:, cols], GU.at[s, k, :, pl.ds(0, width)], r["gus"].at[s, k]) for k, a in enumerate((gate, up))]
        go(copies + [pltpu.make_async_copy(w_down.at[0, cols, :], WD.at[s, pl.ds(0, width)], r["gus"].at[s, 2])], start)

    def put(t, width, start):
        s, cols = lax.rem(t, 2), pl.ds(al(t * BLOCK, LANES), width)
        go([pltpu.make_async_copy(DS.at[s, :, pl.ds(0, width)], by_up0.at[:, cols], r["dus"].at[s])], start)

    barrier = pltpu.get_barrier_semaphore()
    for d in range(SIX):
        pl.semaphore_signal(barrier, inc=1, device_id=at(across(d)[0]), device_id_type=MESH)
    pl.semaphore_signal(barrier, inc=1, device_id=at(partner), device_id_type=MESH)
    left(dy_t, 0).start()
    colors(lambda j, slabs: right(0, j, slabs).start())
    left(a1_t, 1).start()
    dy_in = pltpu.make_async_copy(dy, BY, r["hs"].at[0])
    h_in = pltpu.make_async_copy(h1, L.at[0], r["hs"].at[1])
    dy_in.start()
    row_tile(0, 0).start()
    hidden(0, BLOCK, START)
    hidden(1, BLOCK, START)
    comm.tables()
    r["SQ"][0] = jnp.zeros((8, LANES), jnp.float32)
    for b in range(4):
        DA[BLOCK * b : BLOCK * b + BLOCK] = jnp.zeros((BLOCK, SIDE), jnp.float32)
    pl.semaphore_wait(barrier, 7)

    def dot(m, row, rows, j, slabs):
        return jnp.dot(
            L[left_of[m], pl.ds(al(row, BLOCK), rows), :],
            X[:, pl.ds(al(j * TILE, TILE), LANES * slabs)],
            preferred_element_type=jnp.float32,
        )

    def theirs(m):
        if m == 0:
            left(dy_t, 0).wait()
        if m == 1:
            left(a1_t, 1).wait()
        if m == 4:
            left(a0_t, 1).wait()
        if m:
            pl.semaphore_wait(r["pcredit"], 1)

        def body(j, slabs):
            n = TILE * slabs
            if m != 4:
                right(m, j, slabs).wait()
            if m:
                for h in range(2):
                    comm.pair(m, j, n, h, partner).wait_send()
            res = dot(m, (1 - core) * TILE, TILE, j, slabs).astype(jnp.bfloat16)
            for h in range(2):
                for s in range(slabs):
                    OUT[pl.ds(al(h * QUARTER + j * SIDE + s * BLOCK), BLOCK)] = res[h * BLOCK : h * BLOCK + BLOCK, s * LANES : s * LANES + LANES]
                comm.pair(m, j, n, h, partner).start()

        colors(body)

    def ours(m):
        slot = m % SLOTS
        if m >= SLOTS:
            for d in range(SIX):
                pl.semaphore_wait(r["credit"].at[d], 1)

        @pl.loop(0, 2)
        def _(stays):
            def body(j, slabs):
                n = TILE * slabs
                device, side = comm.other(m, j, 1), comm.side(m, j, 1)
                h = stays * side + (1 - stays) * (1 - side)
                comm.pair(m, j, n, h, partner).wait_recv()
                res = dot(m, core * TILE + h * BLOCK, BLOCK, j, slabs)

                def total(s):
                    return res[:, s * LANES : s * LANES + LANES] + RP[pl.ds(al(h * QUARTER + j * SIDE + s * BLOCK), BLOCK)].astype(jnp.float32)

                @pl.when(stays == 0)
                def _():
                    for s in range(slabs):
                        O[slot, pl.ds(al(comm.sent(j, n, 1) + s * BLOCK), BLOCK)] = total(s).astype(jnp.bfloat16)
                    comm.rdma(m, j, n, 1, device).start()

                @pl.when(stays == 1)
                def _():
                    for s in range(slabs):
                        F[slot, pl.ds(al(j * SIDE + s * BLOCK), BLOCK)] = total(s)
                    if m in (0, 4):
                        right(m + 1, j, slabs).start()

            colors(body)

        if m < 5:
            pl.semaphore_signal(r["pcredit"], inc=1, device_id=at(partner), device_id_type=MESH)
        if m == 0:
            h_in.start()
        if m == 2:
            left(a0_t, 1).start()

    def by_normed(i):
        which, part = divmod(i, 3)

        def body(j, slabs):
            cols = pl.ds(al(j * TILE, LANES), LANES * slabs)
            row_tile(which, j).wait()
            if isinstance(j, int):
                if which == 0:
                    row_tile(1, 0).start()
            else:
                row_tile(which, j + 1).start()
            for half in range(2):
                rows = slice(TILE * half, TILE * half + TILE)
                part_of = dot_t(X[rows, cols], WT[lax.rem(j, 2), :, 0 : LANES * slabs])
                DA[rows] += part_of
            right(2 + which, j, slabs).start()

        if part == 2:
            body(5, 5)
        else:

            @pl.loop(3 * part, 3 + 2 * part)
            def _(j):
                body(j, 4)

    def normed_back():
        dy_in.wait()
        h_in.wait()

        @pl.loop(0, 8)
        def _(b):
            rows = pl.ds(al(b * LANES, LANES), LANES)
            wide = L[0, rows].astype(jnp.float32)
            scale = scale_of(wide)
            d = DA[rows].astype(jnp.bfloat16).astype(jnp.float32)
            through = d * scale - wide * (scale * scale * scale * jnp.mean(d * wide, -1, keepdims=START))
            BY[rows] = BY[rows] + through.astype(jnp.bfloat16)

        @pl.loop(0, 8)
        def _(b):
            rows = pl.ds(al(b * LANES, LANES), LANES)
            L[0, :, rows] = BY[rows].T

    def by_hidden(i):
        def body(t, width):
            s = lax.rem(t, 2)
            hidden(t, width, WAIT)

            @pl.when(t >= 2)
            def _():
                put(t - 2, BLOCK, WAIT)

            @pl.loop(0, 2)
            def _(half):
                rows = pl.ds(al(half * TILE, TILE), TILE)
                d = dot_t(BY[rows], WD[s, 0:width]).astype(jnp.bfloat16).astype(jnp.float32)
                gt = GU[s, 0, rows, 0:width]
                sig = jax.nn.sigmoid(gt)
                X[rows, pl.ds(al(t * BLOCK, LANES), width)] = (d * GU[s, 1, rows, 0:width] * (sig * (1 + gt * (1 - sig)))).astype(jnp.bfloat16)
                DS[s, rows, 0:width] = (d * (gt * sig)).astype(jnp.bfloat16)

            put(t, width, START)
            if width == BLOCK:

                @pl.when(t < 10)
                def _():
                    hidden(t + 2, BLOCK, START)

                @pl.when(t == 10)
                def _():
                    hidden(12, LANES, START)

        if i < 3:

            @pl.loop(4 * i, 4 * i + 4)
            def _(t):
                body(t, BLOCK)

        else:
            body(jnp.int32(12), LANES)
            put(11, BLOCK, WAIT)
            put(12, LANES, WAIT)

    def run(kind, m, k):
        if kind == "theirs":
            theirs(m)
        elif kind == "ours":
            ours(m)
        elif kind == "normed":
            by_normed(m)
        elif kind == "back_normed":
            normed_back()
        elif kind == "hidden":
            by_hidden(m)
        elif kind == "add":
            comm.add(m, k)
        elif kind == "back":
            comm.back(m, k)
        elif kind == "free":
            comm.free(m)
        elif kind == "sq":
            comm.squares(m)

    for item in order:
        if SCOPES:
            with jax.named_scope("_".join(str(i) for i in item)):
                run(*item)
        else:
            run(*item)
    for m in range(SIX):
        comm.finish(m)

    def last(j, slabs):
        for h in range(2):
            comm.pair(5, j, TILE * slabs, h, partner).wait_send()

    colors(last)
    total = jnp.sum(jnp.sum(r["SQ"][7], 1, keepdims=START), 0, keepdims=START)
    count = SIX * ROWS * LANES
    factor[...] = jnp.broadcast_to(jnp.minimum(1.0, 0.5 * lax.rsqrt(total / count + 1e-30)), (8, LANES))


def summed_gradients(order, *args):
    dma = pltpu.SemaphoreType.DMA
    regular = pltpu.SemaphoreType.REGULAR
    return pl.pallas_call(
        functools.partial(gradients_kernel, order=order),
        out_shape=(jax.ShapeDtypeStruct((SIX * ROWS, LANES), jnp.bfloat16), jax.ShapeDtypeStruct((8, LANES), jnp.float32), jax.ShapeDtypeStruct((SIDE, WIDE), jnp.bfloat16)),
        in_specs=[ANY] * 14,
        out_specs=[ANY, pl.BlockSpec(memory_space=pltpu.VMEM), ANY],
        scratch_shapes=[pltpu.VMEM(shape, t) for _, shape, t in SCRATCH] + [dma(shape) for _, shape in SEMAPHORES] + [regular((SIX,)), regular((SIX,)), regular],
        compiler_params=pltpu.CompilerParams(collective_id=0, has_side_effects=START, vmem_limit_bytes=67043328),
        name="gradients",
    )(*args)


CHOICES = (
    182964243178488320, 59396926352994440, 505397359579086987, 681682808683529988,
    1116504966391876526, 114749310,
)


def steps():
    compute = []
    for m in range(SIX):
        compute += [(kind, m, -1) for kind in ("theirs", "ours")]
        if m in (1, 2):
            compute += [("normed", 3 * m - 3 + i, -1) for i in range(3)]
        if m == 2:
            compute.append(("back_normed", 0, -1))
        if m == 3:
            compute += [("hidden", i, -1) for i in range(4)]
    chains = [compute]
    for m in range(SIX):
        chains.append([("add", m, k) for k in range(1, 7)] + [("back", m, k) for k in range(5, -1, -1)] + [("free", m, 0)])
    chains.append([("sq", i, 0) for i in range(8)])
    chains = [iter(chain) for chain in chains]
    count = 109
    return [next(chains[CHOICES[i // 20] >> (3 * (i % 20)) & 7]) for i in range(count)]


ROWS_A = 64
DEEP = 4


def adam_kernel(factor, g, *refs):
    ins, outs = (refs[0:3], refs[3:SIX], refs[SIX:9]), (refs[9:12], refs[12:15], refs[15:18])
    gf, gt, *rest = refs[18:]
    flat_in, turned_in, flat_out, turned_out, got, put = rest[0:3], rest[3:SIX], rest[SIX:9], rest[9:12], rest[12], rest[13]
    per = SIDE // ROWS_A
    flat, tiles = 4 * per, 4 * per + 50

    def pieces(i, act):
        for n in range(3):
            first, count = (0, per) if n == 0 else (2 * per, per) if n == 1 else (4 * per, 25)

            @pl.when((i >= first) & (i < first + 2 * count))
            def _():
                layer, t = lax.div(i - first, count), lax.rem(i - first, count)
                chunk = (layer * (2 - n) + (1 - layer) * (4, 5, 3)[n]) * 4
                rows = LANES if n == 2 else ROWS_A
                place = (layer, pl.ds(pl.multiple_of(t * rows, rows), rows))
                if n == 2:
                    act(n, place, g.at[pl.ds(chunk, 4), t])
                else:
                    part = BLOCK // ROWS_A
                    act(n, place, g.at[chunk + lax.div(t, part), :, pl.ds(pl.multiple_of(lax.rem(t, part) * ROWS_A, ROWS_A), ROWS_A)])

    def load(i, start):
        slot = lax.rem(i, DEEP)

        def act(n, place, grads):
            copies = [pltpu.make_async_copy(grads, (gt if n == 2 else gf).at[slot], got.at[slot, 3])]
            for k in range(3):
                buffer = (turned_in if n == 2 else flat_in)[k]
                copies.append(pltpu.make_async_copy(ins[k][n].at[place], buffer.at[slot], got.at[slot, k]))
            for c in copies:
                c.start() if start else c.wait()

        pieces(i, act)

    def store(i, start):
        slot = lax.rem(i, DEEP)

        def act(n, place, grads):
            for k in range(3):
                buffer = (turned_out if n == 2 else flat_out)[k]
                c = pltpu.make_async_copy(buffer.at[slot], outs[k][n].at[place], put.at[slot, k])
                c.start() if start else c.wait()

        pieces(i, act)

    def compute(i, turned):
        slot = lax.rem(i, DEEP)
        w, m, v = turned_in if turned else flat_in
        w_out, m_out, v_out = turned_out if turned else flat_out
        f = factor[0:1, 0:1] if turned else factor[0:1, :]

        def part(s):
            if turned:
                piece = gt[slot, s].astype(jnp.float32).T
                where = (slot, slice(None), pl.ds(pl.multiple_of(BLOCK * s, BLOCK), BLOCK))
            else:
                piece = gf[slot, s].astype(jnp.float32)
                where = (slot, slice(None), pl.ds(pl.multiple_of(LANES * s, LANES), LANES))
            piece = piece * f
            new_m = 0.9 * m[where] + 0.1 * piece
            new_v = 0.95 * v[where] + 0.05 * piece * piece
            wide = w[where].astype(jnp.float32)
            step = new_m * lax.rsqrt(new_v + 1e-8) + 0.1 * wide
            m_out[where] = new_m
            v_out[where] = new_v
            w_out[where] = (wide - 0.02 * step).astype(jnp.bfloat16)

        if turned:
            pl.loop(0, 4)(part)
        else:

            @pl.loop(0, 5)
            def _(i):
                for s in range(5):
                    part(5 * i + s)

    @pl.loop(0, DEEP - 1)
    def _(i):
        load(i, START)


    @pl.loop(0, tiles)
    def _(i):
        @pl.when(i + DEEP - 1 < tiles)
        def _():
            load(i + DEEP - 1, START)

        load(i, WAIT)

        @pl.when(i >= DEEP)
        def _():
            store(i - DEEP, WAIT)

        @pl.when(i < flat)
        def _():
            compute(i, WAIT)

        @pl.when(i >= flat)
        def _():
            compute(i, START)

        store(i, START)

    @pl.loop(tiles - DEEP, tiles)
    def _(i):
        store(i, WAIT)


def adam(factor, g, weights, m, v):
    arrays = (*weights, *m, *v)
    flat, turned = (DEEP, ROWS_A, WIDE), (DEEP, LANES, SIDE)
    types = (jnp.bfloat16, jnp.float32, jnp.float32)
    return pl.pallas_call(
        adam_kernel,
        out_shape=tuple(jax.ShapeDtypeStruct(a.shape, a.dtype) for a in arrays),
        in_specs=[pl.BlockSpec(memory_space=pltpu.VMEM), ANY] + [ANY] * 9,
        out_specs=(ANY,) * 9,
        scratch_shapes=[pltpu.VMEM((DEEP, 25, ROWS_A, LANES), jnp.bfloat16), pltpu.VMEM((DEEP, 4, BLOCK, LANES), jnp.bfloat16)]
        + [pltpu.VMEM(shape, t) for _ in range(2) for shape in (flat, turned) for t in types]
        + [pltpu.SemaphoreType.DMA((DEEP, 4)), pltpu.SemaphoreType.DMA((DEEP, 3))],
        compiler_params=pltpu.CompilerParams(vmem_limit_bytes=60 * 2**20),
        name="adam",
    )(factor, g.reshape(24, 25, BLOCK, LANES), *arrays)


def solution(mesh):
    order = steps()

    def step(x, dy, *arrays):
        weights, m, v = (arrays[i : i + 3] for i in (0, 3, SIX))
        g, factor, _ = summed_gradients(order, *forward(x[0], dy[0], *weights))
        return tuple(adam(factor, g, weights, m, v))

    return jax.shard_map(
        step,
        mesh=mesh,
        in_specs=(P(("rep", "dp"), None, None),) * 2 + (P(None, None, None),) * 9,
        out_specs=(P("rep", None, None),) * 9,
        check_vma=WAIT,
    )
```
